128 devices in a mesh: ep: 32 (over y, z, core), dp: 4 (over x).
Axes of the slice: x: 4, y: 4, z: 4, core: 2. Of those that a mesh axis runs over, the one named last changes fastest.
Arguments:
- lengths: int32 [128, 16], P(('ep', 'dp')), may hold values from 1 to 512, as said below
- id_lists: int32 [128, 16, 512], P(('ep', 'dp')), may hold values from 0 to 65535, as said below
- feature_slots: int32 [16], replicated, may hold values from 0 to 15, each once
- embedding_table: bfloat16 [1048576, 128], P(('ep', 'dp')), may hold values from -6 to 6
Outputs:
- embedded: bfloat16 [128, 16, 512, 128], P(('ep', 'dp'))
The draws below stay inside these ranges and needn't reach their ends.
Inputs may be any that keep to these rules, and one draw needn't show every extreme that they name: `lengths`: every user has some feature whose length is exactly 512. `id_lists`: among the valid entries (positions below the list's length) of the 1 users of one device, at most 80 ids lie in any one block of 512 ids that starts at a multiple of 512; in every draw some block holds exactly 80 valid ids from every device. Entries past a list's length hold arbitrary ids of the range.
All inputs are finite; a program needn't handle non-finite values.
Results may differ from the reference program's by a relative error of at most 0.001.
Values may be sent and summed in bfloat16 or wider, within the bound.
No kernel may reach another device: no remote copies, remote signals or barrier semaphores. Data moves between devices by JAX's collectives and lax.ppermute only.
A program may use at most 64 MiB of HBM per device.

```python
import jax
import jax.numpy as jnp

B_DEV = 1
F = 16
L = 512
E = 128
USERS = 128
ROWS = 1048576
OWNER_IDS = 512
CAP = 80
DEVICES = 128


def make_lists(key):
    slot_total = B_DEV * F * L
    key_len = jax.random.fold_in(key, 101)
    key_full = jax.random.fold_in(key, 202)
    key_hot = jax.random.fold_in(key, 303)
    key_perm = jax.random.fold_in(key, 404)
    key_pad = jax.random.fold_in(key, 505)
    key_local = jax.random.fold_in(key, 606)
    raw_lengths = jax.random.randint(key_len, (USERS, F), 1, L + 1)
    longest = jax.random.randint(key_full, (USERS,), 0, F)
    lengths = jnp.where(jnp.arange(F)[None, :] == longest[:, None], L, raw_lengths).astype(jnp.int32)
    live_mask = (jnp.arange(L)[None, None, :] < lengths[:, :, None]).reshape(DEVICES, slot_total)
    live_rank = jnp.cumsum(live_mask.astype(jnp.int32), axis=1) - 1
    hot_owner = jax.random.randint(key_hot, (), 0, DEVICES)
    shuffled = jax.vmap(lambda sub: jax.random.permutation(sub, slot_total))(jax.random.split(key_perm, DEVICES)).astype(jnp.int32)
    later = jnp.take_along_axis(shuffled, jnp.clip(live_rank - CAP, 0, slot_total - 1), axis=1)
    spread = later % (DEVICES - 1)
    spread = jnp.where(spread >= hot_owner, spread + 1, spread)
    owner_of = jnp.where(live_rank < CAP, hot_owner, spread)
    stray = jax.random.randint(key_pad, (DEVICES, slot_total), 0, DEVICES)
    owner_of = jnp.where(live_mask, owner_of, stray)
    within = jax.random.randint(key_local, (DEVICES, slot_total), 0, OWNER_IDS)
    id_lists = (owner_of * OWNER_IDS + within).reshape(USERS, F, L).astype(jnp.int32)
    return (lengths, id_lists)


def draw_lengths(key, part):
    return make_lists(key)[0]


def draw_id_lists(key, part):
    return make_lists(key)[1]


def block_scale(rng, dims, pieces, smallest, top_value):
    factor_of, own = 1.0, jax.random.fold_in(rng, 6)
    for axis_at, shards_of in pieces:
        steps = jnp.exp(jax.random.uniform(jax.random.fold_in(own, axis_at), (shards_of,), jnp.float32, smallest / len(pieces), top_value / len(pieces)))
        factor_of = factor_of * jnp.repeat(steps, dims[axis_at] // shards_of).reshape([-1 if axis == axis_at else 1 for axis in range(len(dims))])
    return factor_of


def bell_draw(key, shape, scale, reach, cuts=(), kind=jnp.bfloat16):
    factor_of = block_scale(key, shape, cuts, -0.22, 0.18) if cuts else 1.0
    values = jax.random.normal(key, shape, jnp.float32) * scale * factor_of
    return jnp.minimum(jnp.maximum(values, -reach), reach).astype(kind)


def setup_inputs(seed: int = 0) -> dict:
    arg_keys = jax.random.split(jax.random.key(seed), 5)
    return {
        "lengths": draw_lengths(jax.random.fold_in(arg_keys[4], 71), 0),
        "id_lists": draw_id_lists(jax.random.fold_in(arg_keys[4], 71), 0),
        "feature_slots": jax.random.permutation(arg_keys[2], F).astype(jnp.int32),
        "embedding_table": bell_draw(arg_keys[3], (ROWS, E), 1.0, 6.0, ((0, 128),)),
    }


def reference(lengths, id_lists, feature_slots, embedding_table):
    stacked = id_lists * F + feature_slots[None, :, None]
    live_mask = jnp.arange(L, dtype=jnp.int32)[None, None, :] < lengths[:, :, None]
    looked_up = jnp.take(embedding_table, stacked, axis=0)
    return jnp.where(live_mask[..., None], looked_up, jnp.zeros((), embedding_table.dtype))
```

```python
import functools

import jax
import jax.numpy as jnp
from jax import lax
from jax.experimental import pallas as pl
from jax.experimental.pallas import tpu as pltpu
from jax.sharding import PartitionSpec as P

LANES = 128
BLOCK = 256


def rank_kernel(per_owner, capacity, len_ref, slot_ref, ids_ref, req_ref, tgt_ref):
    feats, span = ids_ref.shape
    owners = req_ref.shape[0]
    owner_row = lax.broadcasted_iota(jnp.int32, (owners, BLOCK), 0)
    rank_row = lax.broadcasted_iota(jnp.int32, (capacity, BLOCK), 0).astype(jnp.float32)
    earlier = lax.broadcasted_iota(jnp.int32, (BLOCK, BLOCK + LANES), 0)
    later = lax.broadcasted_iota(jnp.int32, (BLOCK, BLOCK + LANES), 1)
    before_of = jnp.where(earlier < later, 1.0, 0.0).astype(jnp.bfloat16)
    lane = lax.broadcasted_iota(jnp.int32, (1, BLOCK), 1)
    offset = jnp.zeros((owners, LANES), jnp.float32)
    request = jnp.zeros((owners, capacity), jnp.float32)
    for f in range(feats):
        for at in range(0, span, BLOCK):
            ids = ids_ref[f : f + 1, at : at + BLOCK]
            valid = (lane + at) < len_ref[0, f]
            owner = ids // per_owner
            hot = owner_row == jnp.where(valid, owner, -1)
            hot_half = jnp.where(hot, 1.0, 0.0).astype(jnp.bfloat16)
            counted = jnp.dot(hot_half, before_of, preferred_element_type=jnp.float32)
            before = counted[:, :BLOCK] + jnp.concatenate([offset] * (BLOCK // LANES), axis=1)
            rank = jnp.sum(jnp.where(hot, before, 0.0), axis=0, keepdims=True)
            offset = offset + counted[:, BLOCK:]
            row = (ids - owner * per_owner) * feats + slot_ref[f]
            high = (row // 128).astype(jnp.float32)
            low = (row % 128).astype(jnp.float32)
            rank_hot = rank_row == rank
            ranked = jnp.concatenate(
                [
                    jnp.where(rank_hot, 128.0, 0.0).astype(jnp.bfloat16),
                    jnp.where(rank_hot, 1.0, 0.0).astype(jnp.bfloat16),
                ],
                axis=1,
            )
            weighted = jnp.concatenate(
                [
                    jnp.where(hot, high, 0.0).astype(jnp.bfloat16),
                    jnp.where(hot, low, 0.0).astype(jnp.bfloat16),
                ],
                axis=1,
            )
            request = request + lax.dot_general(
                weighted, ranked, (((1,), (1,)), ((), ())), preferred_element_type=jnp.float32
            )
            slot = owner * capacity + rank.astype(jnp.int32)
            tgt_ref[f : f + 1, at : at + BLOCK] = jnp.where(valid, slot, owners * capacity)
    req_ref[...] = request.astype(jnp.int32)


def widen(dst_ref, src_ref, step=256):
    def convert(i, _):
        at = pl.multiple_of(i * step, step)
        dst_ref[pl.ds(at, step), :] = src_ref[pl.ds(at, step), :].astype(jnp.float32)
        return 0

    lax.fori_loop(0, src_ref.shape[0] // step, convert, 0)


def lookup_kernel(inc_ref, tab_ref, out_ref, wide, stage):
    widen(wide, tab_ref)

    def body(d, _):
        for r in range(out_ref.shape[1]):
            stage[r : r + 1, :] = wide[pl.ds(inc_ref[d, r], 1), :]
        out_ref[d] = stage[...].astype(out_ref.dtype)
        return 0

    lax.fori_loop(0, out_ref.shape[0], body, 0)


def place_kernel(tgt_ref, ret_ref, out_ref, wide, stage):
    slots = ret_ref.shape[0]
    span = out_ref.shape[1]
    group = stage.shape[0]
    widen(wide, ret_ref)
    wide[slots:, :] = jnp.zeros((wide.shape[0] - slots, wide.shape[1]), jnp.float32)

    def body(k, _):
        f = k // (span // group)
        at = pl.multiple_of((k % (span // group)) * group, group)
        for r in range(group):
            stage[r : r + 1, :] = wide[pl.ds(tgt_ref[f, at + r], 1), :]
        out_ref[f, pl.ds(at, group), :] = stage[...].astype(out_ref.dtype)
        return 0

    lax.fori_loop(0, out_ref.shape[0] * (span // group), body, 0)


def on_device(lengths, id_lists, feature_slots, embedding_table):
    num_users, num_feats, list_span = id_lists.shape
    row_width = embedding_table.shape[1]
    owners = lax.axis_size("ep") * lax.axis_size("dp")
    per_owner = embedding_table.shape[0] // num_feats
    slot_total = num_users * num_feats * list_span
    capacity = 5 * slot_total // (4 * owners)
    axes = ("ep", "dp")
    smem = pl.BlockSpec(memory_space=pltpu.SMEM)
    vmem = pl.BlockSpec(memory_space=pltpu.VMEM)

    request, targets = pl.pallas_call(
        functools.partial(rank_kernel, per_owner, capacity),
        out_shape=(
            jax.ShapeDtypeStruct((owners, capacity), jnp.int32),
            jax.ShapeDtypeStruct((num_feats, list_span), jnp.int32),
        ),
        in_specs=[smem, smem, vmem],
        out_specs=(vmem, vmem),
        name="rank_ids",
    )(lengths, feature_slots, id_lists.reshape(num_feats, list_span))
    incoming = lax.all_to_all(request, axes, split_axis=0, concat_axis=0, tiled=True)
    replies = pl.pallas_call(
        lookup_kernel,
        out_shape=jax.ShapeDtypeStruct((owners, capacity, row_width), embedding_table.dtype),
        in_specs=[smem, vmem],
        out_specs=vmem,
        scratch_shapes=[
            pltpu.VMEM(embedding_table.shape, jnp.float32),
            pltpu.VMEM((capacity, row_width), jnp.float32),
        ],
        name="lookup_rows",
    )(incoming, embedding_table)
    returned = lax.all_to_all(replies, axes, split_axis=0, concat_axis=0, tiled=True)
    returned = returned.reshape(owners * capacity, row_width)
    embedded = pl.pallas_call(
        place_kernel,
        out_shape=jax.ShapeDtypeStruct((num_feats, list_span, row_width), embedding_table.dtype),
        in_specs=[smem, vmem],
        out_specs=vmem,
        scratch_shapes=[
            pltpu.VMEM((owners * capacity + 8, row_width), jnp.float32),
            pltpu.VMEM((64, row_width), jnp.float32),
        ],
        name="place_rows",
    )(targets, returned)
    return embedded.reshape(num_users, num_feats, list_span, row_width)


def solution(mesh):
    placed = (P(("ep", "dp"), None), P(("ep", "dp"), None, None), P(), P(("ep", "dp"), None))
    return jax.shard_map(
        on_device,
        mesh=mesh,
        in_specs=placed,
        out_specs=P(("ep", "dp"), None, None, None),
        check_vma=False,
    )
```

```python
import functools

import jax
import jax.numpy as jnp
from jax import lax
from jax.experimental import pallas as pl
from jax.experimental.pallas import tpu as pltpu
from jax.sharding import PartitionSpec as P

LANES = 128
BLOCK = 256
GROUP = 16
WINDOW = 64
MIB = 2**20


def rank_kernel(
    per_owner,
    capacity,
    len_hbm,
    slot_hbm,
    ids_hbm,
    tab_hbm,
    req_ref,
    tgt_ref,
    wide_ref,
    len_ref,
    slot_ref,
    ids_ref,
    tab_ref,
    sems,
):
    copies = [
        pltpu.make_async_copy(src, dst, sems.at[k])
        for k, (src, dst) in enumerate(
            [(len_hbm, len_ref), (slot_hbm, slot_ref), (ids_hbm, ids_ref), (tab_hbm, tab_ref)]
        )
    ]
    for copy in copies:
        copy.start()
    feats, span = ids_ref.shape
    owners = req_ref.shape[0]
    owner_row = lax.broadcasted_iota(jnp.int32, (owners, BLOCK), 0)
    rank_row = lax.broadcasted_iota(jnp.int32, (capacity, BLOCK), 0).astype(jnp.float32)
    earlier = lax.broadcasted_iota(jnp.int32, (BLOCK, BLOCK + LANES), 0)
    later = lax.broadcasted_iota(jnp.int32, (BLOCK, BLOCK + LANES), 1)
    before_of = jnp.where(earlier < later, 1.0, 0.0).astype(jnp.bfloat16)
    lane = lax.broadcasted_iota(jnp.int32, (1, BLOCK), 1)
    offset = jnp.zeros((owners, LANES), jnp.float32)
    request = jnp.zeros((owners, capacity), jnp.float32)
    for copy in copies[:3]:
        copy.wait()
    steps = feats * (span // BLOCK)
    for step in range(steps):
        f, at = step // (span // BLOCK), step % (span // BLOCK) * BLOCK
        ids = ids_ref[f : f + 1, at : at + BLOCK]
        valid = (lane + at) < len_ref[0, f]
        owner = ids // per_owner
        hot = owner_row == jnp.where(valid, owner, -1)
        hot_half = jnp.where(hot, 1.0, 0.0).astype(jnp.bfloat16)
        counted = jnp.dot(hot_half, before_of, preferred_element_type=jnp.float32)
        before = counted[:, :BLOCK] + jnp.concatenate([offset] * (BLOCK // LANES), axis=1)
        rank = jnp.sum(jnp.where(hot, before, 0.0), axis=0, keepdims=True)
        offset = offset + counted[:, BLOCK:]
        row = (ids - owner * per_owner) * feats + slot_ref[f]
        high = (row // 128).astype(jnp.float32)
        low = (row % 128).astype(jnp.float32)
        rank_hot = rank_row == rank
        ranked = jnp.concatenate(
            [
                jnp.where(rank_hot, 128.0, 0.0).astype(jnp.bfloat16),
                jnp.where(rank_hot, 1.0, 0.0).astype(jnp.bfloat16),
            ],
            axis=1,
        )
        weighted = jnp.concatenate(
            [
                jnp.where(hot, high, 0.0).astype(jnp.bfloat16),
                jnp.where(hot, low, 0.0).astype(jnp.bfloat16),
            ],
            axis=1,
        )
        request = request + lax.dot_general(
            weighted, ranked, (((1,), (1,)), ((), ())), preferred_element_type=jnp.float32
        )
        slot = owner * capacity + rank.astype(jnp.int32)
        slot = jnp.where(valid, slot, owners * capacity)
        for part in range(BLOCK // LANES):
            line = f * (span // LANES) + at // LANES + part
            tgt_ref[line : line + 1, :] = slot[:, part * LANES : (part + 1) * LANES]
    copies[3].wait()
    widen(wide_ref, tab_ref)
    req_ref[:, :capacity] = request.astype(jnp.int32)
    req_ref[:, capacity:] = offset[:, capacity:].astype(jnp.int32)


def widen(dst_ref, src_ref, step=256):
    def convert(i, _):
        at = pl.multiple_of(i * step, step)
        dst_ref[pl.ds(at, step), :] = src_ref[pl.ds(at, step), :].astype(jnp.float32)
        return 0

    lax.fori_loop(0, src_ref.shape[0] // step, convert, 0)


def lookup_kernel(capacity, inc_ref, wide_ref, out_ref, stage):
    def body(d, _):
        count = inc_ref[d, capacity]
        for g in range(0, capacity, GROUP):

            @pl.when(count > g)
            def _():
                for r in range(g, g + GROUP):
                    stage[r : r + 1, :] = wide_ref[pl.ds(inc_ref[d, r], 1), :]

        out_ref[d] = stage[...].astype(out_ref.dtype)
        return 0

    lax.fori_loop(0, out_ref.shape[0], body, 0)


def place_kernel(len_ref, tgt_ref, ret_ref, out_hbm, wide, stage, out_ref, sem):
    slots = ret_ref.shape[0]
    feats, span = out_ref.shape[:2]
    widen(wide, ret_ref)
    wide[slots:, :] = jnp.zeros((wide.shape[0] - slots, wide.shape[1]), jnp.float32)
    zeros = jnp.zeros((WINDOW, wide.shape[1]), out_ref.dtype)

    def feature(f, _):
        used = (len_ref[0, f] + (WINDOW - 1)) // WINDOW

        def filled(k, _):
            for h in range(LANES // WINDOW):

                @pl.when(k % (LANES // WINDOW) == h)
                def _():
                    line = f * (span // LANES) + k // (LANES // WINDOW)
                    for r in range(WINDOW):
                        stage[r : r + 1, :] = wide[pl.ds(tgt_ref[line, h * WINDOW + r], 1), :]

            out_ref[f, pl.ds(pl.multiple_of(k * WINDOW, WINDOW), WINDOW), :] = stage[...].astype(out_ref.dtype)
            return 0

        def blank(k, _):
            out_ref[f, pl.ds(pl.multiple_of(k * WINDOW, WINDOW), WINDOW), :] = zeros
            return 0

        lax.fori_loop(0, used, filled, 0)
        lax.fori_loop(used, span // WINDOW, blank, 0)
        pltpu.make_async_copy(out_ref.at[f], out_hbm.at[f], sem).start()
        return 0

    lax.fori_loop(0, feats, feature, 0)
    pltpu.make_async_copy(out_ref, out_hbm, sem).wait()


def on_device(lengths, id_lists, feature_slots, embedding_table):
    num_users, num_feats, list_span = id_lists.shape
    rows, row_width = embedding_table.shape
    owners = lax.axis_size("ep") * lax.axis_size("dp")
    per_owner = rows // num_feats
    slot_total = num_users * num_feats * list_span
    capacity = 5 * slot_total // (4 * owners)
    axes = ("ep", "dp")
    dtype = embedding_table.dtype
    smem = pl.BlockSpec(memory_space=pltpu.SMEM)
    vmem = pl.BlockSpec(memory_space=pltpu.VMEM)
    hbm = pl.BlockSpec(memory_space=pltpu.HBM)
    ids = id_lists.reshape(num_feats, list_span)

    request, targets, wide = pl.pallas_call(
        functools.partial(rank_kernel, per_owner, capacity),
        out_shape=(
            pltpu.VMEM((owners, LANES), jnp.int32),
            pltpu.VMEM((slot_total // LANES, LANES), jnp.int32),
            pltpu.VMEM((rows, row_width), jnp.float32),
        ),
        in_specs=[hbm] * 4,
        out_specs=(vmem,) * 3,
        scratch_shapes=[
            pltpu.SMEM(lengths.shape, jnp.int32),
            pltpu.SMEM(feature_slots.shape, jnp.int32),
            pltpu.VMEM(ids.shape, jnp.int32),
            pltpu.VMEM((rows, row_width), dtype),
            pltpu.SemaphoreType.DMA((4,)),
        ],
        compiler_params=pltpu.CompilerParams(vmem_limit_bytes=16 * MIB),
        name="rank_ids",
    )(*(pltpu.with_memory_space_constraint(x, pltpu.HBM) for x in (lengths, feature_slots, ids, embedding_table)))
    incoming = lax.all_to_all(request, axes, split_axis=0, concat_axis=0, tiled=True)
    replies = pl.pallas_call(
        functools.partial(lookup_kernel, capacity),
        out_shape=jax.ShapeDtypeStruct((owners, capacity, row_width), dtype),
        in_specs=[smem, vmem],
        out_specs=vmem,
        scratch_shapes=[pltpu.VMEM((capacity, row_width), jnp.float32)],
        compiler_params=pltpu.CompilerParams(vmem_limit_bytes=16 * MIB),
        name="lookup_rows",
    )(incoming, wide)
    returned = lax.all_to_all(replies, axes, split_axis=0, concat_axis=0, tiled=True)
    returned = returned.reshape(owners * capacity, row_width)
    embedded = pl.pallas_call(
        place_kernel,
        out_shape=jax.ShapeDtypeStruct((num_feats, list_span, row_width), dtype),
        in_specs=[smem, smem, vmem],
        out_specs=hbm,
        scratch_shapes=[
            pltpu.VMEM((owners * capacity + 8, row_width), jnp.float32),
            pltpu.VMEM((WINDOW, row_width), jnp.float32),
            pltpu.VMEM((num_feats, list_span, row_width), dtype),
            pltpu.SemaphoreType.DMA,
        ],
        compiler_params=pltpu.CompilerParams(vmem_limit_bytes=20 * MIB),
        name="place_rows",
    )(pltpu.with_memory_space_constraint(lengths, pltpu.HBM), targets, returned)
    return embedded.reshape(num_users, num_feats, list_span, row_width)


def solution(mesh):
    placed = (P(("ep", "dp"), None), P(("ep", "dp"), None, None), P(), P(("ep", "dp"), None))
    return jax.shard_map(
        on_device,
        mesh=mesh,
        in_specs=placed,
        out_specs=P(("ep", "dp"), None, None, None),
        check_vma=False,
    )
```

```python
import functools

import jax
import jax.numpy as jnp
from jax import lax
from jax.experimental import pallas as pl
from jax.experimental.pallas import tpu as pltpu
from jax.sharding import PartitionSpec as P

LANES = 128
BLOCK = 256
GROUP = 16
WINDOW = 64
PAD = 8
DEPTH = 4
MIB = 2**20


def rank_kernel(
    per_owner,
    capacity,
    len_hbm,
    slot_hbm,
    ids_hbm,
    tab_hbm,
    req_ref,
    tgt_ref,
    wide_ref,
    len_ref,
    slot_ref,
    ids_ref,
    tab_ref,
    sems,
):
    copies = [
        pltpu.make_async_copy(src, dst, sems.at[k])
        for k, (src, dst) in enumerate(
            [(len_hbm, len_ref), (slot_hbm, slot_ref), (ids_hbm, ids_ref), (tab_hbm, tab_ref)]
        )
    ]
    for copy in copies:
        copy.start()
    feats, span = ids_ref.shape
    owners = req_ref.shape[0]
    owner_row = lax.broadcasted_iota(jnp.int32, (owners, BLOCK), 0)
    rank_row = lax.broadcasted_iota(jnp.int32, (capacity, BLOCK), 0).astype(jnp.float32)
    earlier = lax.broadcasted_iota(jnp.int32, (BLOCK, BLOCK + LANES), 0)
    later = lax.broadcasted_iota(jnp.int32, (BLOCK, BLOCK + LANES), 1)
    before_of = jnp.where(earlier < later, 1.0, 0.0).astype(jnp.bfloat16)
    lane = lax.broadcasted_iota(jnp.int32, (1, BLOCK), 1)
    offset = jnp.zeros((owners, LANES), jnp.float32)
    request = jnp.zeros((owners, capacity), jnp.float32)
    for copy in copies[:3]:
        copy.wait()
    steps = feats * (span // BLOCK)
    for step in range(steps):
        f, at = step // (span // BLOCK), step % (span // BLOCK) * BLOCK
        ids = ids_ref[f : f + 1, at : at + BLOCK]
        valid = (lane + at) < len_ref[0, f]
        owner = ids // per_owner
        hot = owner_row == jnp.where(valid, owner, -1)
        hot_half = jnp.where(hot, 1.0, 0.0).astype(jnp.bfloat16)
        counted = jnp.dot(hot_half, before_of, preferred_element_type=jnp.float32)
        before = counted[:, :BLOCK] + jnp.concatenate([offset] * (BLOCK // LANES), axis=1)
        rank = jnp.sum(jnp.where(hot, before, 0.0), axis=0, keepdims=True)
        offset = offset + counted[:, BLOCK:]
        row = (ids - owner * per_owner) * feats + slot_ref[f]
        high = (row // 128).astype(jnp.float32)
        low = (row % 128).astype(jnp.float32)
        rank_hot = rank_row == rank
        ranked = jnp.concatenate(
            [
                jnp.where(rank_hot, 128.0, 0.0).astype(jnp.bfloat16),
                jnp.where(rank_hot, 1.0, 0.0).astype(jnp.bfloat16),
            ],
            axis=1,
        )
        weighted = jnp.concatenate(
            [
                jnp.where(hot, high, 0.0).astype(jnp.bfloat16),
                jnp.where(hot, low, 0.0).astype(jnp.bfloat16),
            ],
            axis=1,
        )
        request = request + lax.dot_general(
            weighted, ranked, (((1,), (1,)), ((), ())), preferred_element_type=jnp.float32
        )
        slot = owner * capacity + rank.astype(jnp.int32)
        slot = jnp.where(valid, slot, owners * capacity)
        for part in range(BLOCK // LANES):
            line = f * (span // LANES) + at // LANES + part
            tgt_ref[line : line + 1, :] = slot[:, part * LANES : (part + 1) * LANES]
    copies[3].wait()
    widen(wide_ref, tab_ref)
    req_ref[:, :capacity] = request.astype(jnp.int32)
    req_ref[:, capacity:] = jnp.zeros((owners, LANES - capacity), jnp.int32)


def widen(dst_ref, src_ref, step=256):
    def convert(i, _):
        at = pl.multiple_of(i * step, step)
        dst_ref[pl.ds(at + PAD, step), :] = src_ref[pl.ds(at, step), :].astype(jnp.float32)
        return 0

    lax.fori_loop(0, src_ref.shape[0] // step, convert, 0)


def gather_rows(wide_ref, index_of, count):
    sublane = lax.broadcasted_iota(jnp.int32, (8, wide_ref.shape[1]), 0)
    tiles = []
    for base in range(0, count, 8):
        tile = wide_ref[pl.ds(index_of(base) + PAD, 8), :]
        for r in range(1, 8):
            tile = jnp.where(sublane == r, wide_ref[pl.ds(index_of(base + r) + (PAD - r), 8), :], tile)
        tiles.append(tile)
    return jnp.concatenate(tiles, axis=0)


def in_windows(source_ref, buffers, sems, body):
    lines = buffers[0].shape[0]
    windows = source_ref.shape[0] // lines
    depth = len(buffers)

    def fetch(w, b):
        at = pl.multiple_of(w * lines, lines)
        return pltpu.make_async_copy(source_ref.at[pl.ds(at, lines)], buffers[b], sems.at[b])

    for b in range(depth):
        fetch(b, b).start()

    def turn(k, _):
        for b in range(depth):
            w = k * depth + b
            fetch(w, b).wait()
            body(w, buffers[b])

            @pl.when(w + depth < windows)
            def _():
                fetch(w + depth, b).start()

        return 0

    return lambda: lax.fori_loop(0, windows // depth, turn, 0)


def lookup_kernel(inc_ref, wide_ref, out_ref, sems, *buffers):
    capacity = out_ref.shape[1]

    def window(w, index_ref):
        lines = index_ref.shape[0]
        for d in range(lines):
            for g in range(0, capacity, GROUP):
                rows = gather_rows(wide_ref, lambda r: index_ref[d, g + r], GROUP)
                out_ref[w * lines + d, g : g + GROUP, :] = rows.astype(out_ref.dtype)

    in_windows(inc_ref, buffers, sems, window)()


def place_kernel(len_hbm, tgt_ref, ret_ref, out_hbm, len_ref, wide, out_ref, out_sem, len_sem, sems, *buffers):
    slots = ret_ref.shape[0]
    feats, span = out_ref.shape[:2]
    zeros = jnp.zeros((WINDOW, wide.shape[1]), out_ref.dtype)
    lengths_copy = pltpu.make_async_copy(len_hbm, len_ref, len_sem)
    lengths_copy.start()

    def feature(f, index_ref):
        used = len_ref[0, f]
        for at in range(0, span, WINDOW):

            @pl.when(used > at)
            def _():
                for g in range(at, at + WINDOW, GROUP):
                    rows = gather_rows(
                        wide, lambda r: index_ref[(g + r) // LANES, (g + r) % LANES], GROUP
                    )
                    out_ref[f, g : g + GROUP, :] = rows.astype(out_ref.dtype)

            @pl.when(used <= at)
            def _():
                out_ref[f, at : at + WINDOW, :] = zeros

        pltpu.make_async_copy(out_ref.at[f], out_hbm.at[f], out_sem).start()

    run = in_windows(tgt_ref, buffers, sems, feature)
    widen(wide, ret_ref)
    wide[PAD + slots :, :] = jnp.zeros((wide.shape[0] - slots - PAD, wide.shape[1]), jnp.float32)
    lengths_copy.wait()
    run()
    pltpu.make_async_copy(out_ref, out_hbm, out_sem).wait()


def on_device(lengths, id_lists, feature_slots, embedding_table):
    num_users, num_feats, list_span = id_lists.shape
    rows, row_width = embedding_table.shape
    owners = lax.axis_size("ep") * lax.axis_size("dp")
    per_owner = rows // num_feats
    slot_total = num_users * num_feats * list_span
    capacity = 5 * slot_total // (4 * owners)
    axes = ("ep", "dp")
    dtype = embedding_table.dtype
    vmem = pl.BlockSpec(memory_space=pltpu.VMEM)
    hbm = pl.BlockSpec(memory_space=pltpu.HBM)
    ids = id_lists.reshape(num_feats, list_span)

    request, targets, wide = pl.pallas_call(
        functools.partial(rank_kernel, per_owner, capacity),
        out_shape=(
            pltpu.VMEM((owners, LANES), jnp.int32),
            pltpu.VMEM((slot_total // LANES, LANES), jnp.int32),
            pltpu.VMEM((PAD + rows + PAD, row_width), jnp.float32),
        ),
        in_specs=[hbm] * 4,
        out_specs=(vmem,) * 3,
        scratch_shapes=[
            pltpu.SMEM(lengths.shape, jnp.int32),
            pltpu.SMEM(feature_slots.shape, jnp.int32),
            pltpu.VMEM(ids.shape, jnp.int32),
            pltpu.VMEM((rows, row_width), dtype),
            pltpu.SemaphoreType.DMA((4,)),
        ],
        compiler_params=pltpu.CompilerParams(vmem_limit_bytes=16 * MIB),
        name="rank_ids",
    )(*(pltpu.with_memory_space_constraint(x, pltpu.HBM) for x in (lengths, feature_slots, ids, embedding_table)))
    incoming = lax.all_to_all(request, axes, split_axis=0, concat_axis=0, tiled=True)
    replies = pl.pallas_call(
        lookup_kernel,
        out_shape=jax.ShapeDtypeStruct((owners, capacity, row_width), dtype),
        in_specs=[vmem, vmem],
        out_specs=vmem,
        scratch_shapes=[pltpu.SemaphoreType.DMA((DEPTH,))] + [pltpu.SMEM((8, LANES), jnp.int32)] * DEPTH,
        compiler_params=pltpu.CompilerParams(vmem_limit_bytes=16 * MIB),
        name="lookup_rows",
    )(incoming, wide)
    returned = lax.all_to_all(replies, axes, split_axis=0, concat_axis=0, tiled=True)
    returned = returned.reshape(owners * capacity, row_width)
    embedded = pl.pallas_call(
        place_kernel,
        out_shape=jax.ShapeDtypeStruct((num_feats, list_span, row_width), dtype),
        in_specs=[hbm, vmem, vmem],
        out_specs=hbm,
        scratch_shapes=[
            pltpu.SMEM(lengths.shape, jnp.int32),
            pltpu.VMEM((PAD + owners * capacity + 2 * PAD, row_width), jnp.float32),
            pltpu.VMEM((num_feats, list_span, row_width), dtype),
            pltpu.SemaphoreType.DMA,
            pltpu.SemaphoreType.DMA,
            pltpu.SemaphoreType.DMA((DEPTH,)),
        ]
        + [pltpu.SMEM((list_span // LANES, LANES), jnp.int32)] * DEPTH,
        compiler_params=pltpu.CompilerParams(vmem_limit_bytes=20 * MIB),
        name="place_rows",
    )(pltpu.with_memory_space_constraint(lengths, pltpu.HBM), targets, returned)
    return embedded.reshape(num_users, num_feats, list_span, row_width)


def solution(mesh):
    placed = (P(("ep", "dp"), None), P(("ep", "dp"), None, None), P(), P(("ep", "dp"), None))
    return jax.shard_map(
        on_device,
        mesh=mesh,
        in_specs=placed,
        out_specs=P(("ep", "dp"), None, None, None),
        check_vma=False,
    )
```

```python
import functools

import jax
import jax.numpy as jnp
from jax import lax
from jax.experimental import pallas as pl
from jax.experimental.pallas import tpu as pltpu
from jax.sharding import PartitionSpec as P

LANES = 128
BLOCK = 256
GROUP = 16
WINDOW = 256
PAD = 8
DEPTH = 4
CHAIN = 8
MIB = 2**20


def rank_kernel(
    per_owner,
    capacity,
    len_hbm,
    slot_hbm,
    ids_hbm,
    tab_hbm,
    req_ref,
    tgt_ref,
    tab_ref,
    len_ref,
    slot_ref,
    ids_ref,
    sems,
):
    copies = [
        pltpu.make_async_copy(src, dst, sems.at[k])
        for k, (src, dst) in enumerate(
            [(len_hbm, len_ref), (slot_hbm, slot_ref), (ids_hbm, ids_ref), (tab_hbm, tab_ref)]
        )
    ]
    for copy in copies:
        copy.start()
    feats, span = ids_ref.shape
    owners = req_ref.shape[0]
    half = jnp.bfloat16
    one, zero = jnp.ones((16, BLOCK), half), jnp.zeros((16, BLOCK), half)
    row_of = lax.broadcasted_iota(jnp.int32, (16, BLOCK), 0).astype(jnp.float32)
    owner_rows = [(row_of + 16 * t).astype(half) for t in range(owners // 16)]
    rank_rows = [(row_of + (16 * t + 1)).astype(half) for t in range(capacity // 16)]
    earlier = lax.broadcasted_iota(jnp.int32, (BLOCK, BLOCK), 0)
    later = lax.broadcasted_iota(jnp.int32, (BLOCK, BLOCK), 1)
    up_to = jnp.where(earlier <= later, 1.0, 0.0).astype(half)
    feature = lax.broadcasted_iota(jnp.int32, (feats, LANES), 0)
    lane = lax.broadcasted_iota(jnp.int32, (feats, span), 1)
    for copy in copies[:3]:
        copy.wait()
    length = jnp.zeros((feats, LANES), jnp.int32)
    slot = jnp.zeros((feats, LANES), jnp.int32)
    for f in range(feats):
        length = jnp.where(feature == f, len_ref[0, f], length)
        slot = jnp.where(feature == f, slot_ref[f], slot)
    ids = ids_ref[...]
    valid = lane < jnp.concatenate([length] * (span // LANES), axis=1)
    owner = ids >> (per_owner.bit_length() - 1)
    row = (ids & (per_owner - 1)) * feats + jnp.concatenate([slot] * (span // LANES), axis=1)
    base = jnp.where(valid, owner * capacity - 1, owners * capacity).astype(jnp.float32)
    owner = jnp.where(valid, owner, -1).astype(jnp.float32)
    high, low = (row >> 7).astype(jnp.float32), (row & 127).astype(jnp.float32)

    offset = [jnp.zeros((16, LANES), half) for _ in owner_rows]
    request = jnp.zeros((owners, 2 * capacity), jnp.float32)
    per_feature = span // BLOCK
    for first in range(0, feats * per_feature, CHAIN):
        hots, wanted = [], []
        for step in range(first, first + CHAIN):
            f, at = step // per_feature, step % per_feature * BLOCK

            def spread(x):
                return jnp.broadcast_to(x, (16, BLOCK)).astype(half)

            def line(x):
                return x[f : f + 1, at : at + BLOCK]

            key = spread(line(owner))
            hot = [jnp.where(rows == key, one, zero) for rows in owner_rows]
            hots.append(jnp.concatenate(hot, axis=0))
            counted = jnp.dot(hots[-1], up_to, preferred_element_type=jnp.float32)
            total = jnp.broadcast_to(counted[:, BLOCK - 1 :], (owners, LANES)).astype(half)
            counted = counted.astype(half)
            picked = zero
            for t in range(len(hot)):
                at_t = slice(16 * t, 16 * t + 16)
                before = counted[at_t] + jnp.concatenate([offset[t]] * (BLOCK // LANES), axis=1)
                picked = picked + hot[t] * before
                offset[t] = offset[t] + total[at_t]
            rank = jnp.sum(picked.astype(jnp.float32), axis=0, keepdims=True)
            key, high_of, low_of = spread(rank), spread(line(high)), spread(line(low))
            found = [rows == key for rows in rank_rows]
            wanted.append(
                jnp.concatenate(
                    [jnp.where(x, high_of, zero) for x in found]
                    + [jnp.where(x, low_of, zero) for x in found],
                    axis=0,
                )
            )
            place = (line(base) + rank).astype(jnp.int32)
            for part in range(BLOCK // LANES):
                at_line = f * (span // LANES) + at // LANES + part
                tgt_ref[at_line : at_line + 1, :] = place[:, part * LANES : (part + 1) * LANES]
        request = request + lax.dot_general(
            jnp.concatenate(hots, axis=1),
            jnp.concatenate(wanted, axis=1),
            (((1,), (1,)), ((), ())),
            preferred_element_type=jnp.float32,
        )
    asked = request[:, :capacity] * 128.0 + request[:, capacity:]
    req_ref[:, :capacity] = asked.astype(jnp.int32)
    req_ref[:, capacity:] = jnp.zeros((owners, LANES - capacity), jnp.int32)
    copies[3].wait()


def widen(dst_ref, src_ref, step=256):
    def convert(i, _):
        at = pl.multiple_of(i * step, step)
        dst_ref[pl.ds(at + PAD, step), :] = src_ref[pl.ds(at, step), :].astype(jnp.float32)
        return 0

    lax.fori_loop(0, src_ref.shape[0] // step, convert, 0)


def gather_rows(wide_ref, index_of, count):
    sublane = lax.broadcasted_iota(jnp.int32, (8, wide_ref.shape[1]), 0)
    tiles = []
    for base in range(0, count, 8):
        tile = wide_ref[pl.ds(index_of(base) + PAD, 8), :]
        for r in range(1, 8):
            tile = jnp.where(sublane == r, wide_ref[pl.ds(index_of(base + r) + (PAD - r), 8), :], tile)
        tiles.append(tile)
    return jnp.concatenate(tiles, axis=0)


def in_windows(source_ref, buffers, sems, body):
    lines = buffers[0].shape[0]
    windows = source_ref.shape[0] // lines
    depth = len(buffers)

    def fetch(w, b):
        at = pl.multiple_of(w * lines, lines)
        return pltpu.make_async_copy(source_ref.at[pl.ds(at, lines)], buffers[b], sems.at[b])

    for b in range(depth):
        fetch(b, b).start()

    def turn(k, _):
        for b in range(depth):
            w = k * depth + b
            fetch(w, b).wait()
            body(w, buffers[b])

            @pl.when(w + depth < windows)
            def _():
                fetch(w + depth, b).start()

        return 0

    return lambda: lax.fori_loop(0, windows // depth, turn, 0)


def lookup_kernel(inc_ref, tab_ref, out_ref, wide_ref, sems, *buffers):
    capacity = out_ref.shape[1]

    def window(w, index_ref):
        lines = index_ref.shape[0]
        for d in range(lines):
            for g in range(0, capacity, GROUP):
                rows = gather_rows(wide_ref, lambda r: index_ref[d, g + r], GROUP)
                out_ref[w * lines + d, g : g + GROUP, :] = rows.astype(out_ref.dtype)

    run = in_windows(inc_ref, buffers, sems, window)
    widen(wide_ref, tab_ref)
    run()


def place_kernel(len_hbm, tgt_ref, ret_ref, out_hbm, len_ref, wide, out_ref, out_sem, len_sem, sems, *buffers):
    slots = ret_ref.shape[0]
    feats, span = out_ref.shape[:2]
    zeros = jnp.zeros((WINDOW, wide.shape[1]), out_ref.dtype)
    lengths_copy = pltpu.make_async_copy(len_hbm, len_ref, len_sem)
    lengths_copy.start()

    def feature(f, index_ref):
        used = len_ref[0, f]
        for at in range(0, span, WINDOW):

            @pl.when(used > at)
            def _():
                for g in range(at, at + WINDOW, GROUP):
                    rows = gather_rows(
                        wide, lambda r: index_ref[(g + r) // LANES, (g + r) % LANES], GROUP
                    )
                    out_ref[f, g : g + GROUP, :] = rows.astype(out_ref.dtype)

            @pl.when(used <= at)
            def _():
                out_ref[f, at : at + WINDOW, :] = zeros

        pltpu.make_async_copy(out_ref.at[f], out_hbm.at[f], out_sem).start()

    run = in_windows(tgt_ref, buffers, sems, feature)
    widen(wide, ret_ref)
    wide[PAD + slots :, :] = jnp.zeros((wide.shape[0] - slots - PAD, wide.shape[1]), jnp.float32)
    lengths_copy.wait()
    run()
    pltpu.make_async_copy(out_ref, out_hbm, out_sem).wait()


def on_device(lengths, id_lists, feature_slots, embedding_table):
    num_users, num_feats, list_span = id_lists.shape
    rows, row_width = embedding_table.shape
    owners = lax.axis_size("ep") * lax.axis_size("dp")
    per_owner = rows // num_feats
    slot_total = num_users * num_feats * list_span
    capacity = 5 * slot_total // (4 * owners)
    axes = ("ep", "dp")
    dtype = embedding_table.dtype
    vmem = pl.BlockSpec(memory_space=pltpu.VMEM)
    hbm = pl.BlockSpec(memory_space=pltpu.HBM)
    ids = id_lists.reshape(num_feats, list_span)

    request, targets, table = pl.pallas_call(
        functools.partial(rank_kernel, per_owner, capacity),
        out_shape=(
            pltpu.VMEM((owners, LANES), jnp.int32),
            pltpu.VMEM((slot_total // LANES, LANES), jnp.int32),
            pltpu.VMEM((rows, row_width), dtype),
        ),
        in_specs=[hbm] * 4,
        out_specs=(vmem,) * 3,
        scratch_shapes=[
            pltpu.SMEM(lengths.shape, jnp.int32),
            pltpu.SMEM(feature_slots.shape, jnp.int32),
            pltpu.VMEM(ids.shape, jnp.int32),
            pltpu.SemaphoreType.DMA((4,)),
        ],
        compiler_params=pltpu.CompilerParams(vmem_limit_bytes=16 * MIB),
        name="rank_ids",
    )(*(pltpu.with_memory_space_constraint(x, pltpu.HBM) for x in (lengths, feature_slots, ids, embedding_table)))
    incoming = lax.all_to_all(request, axes, split_axis=0, concat_axis=0, tiled=True)
    replies = pl.pallas_call(
        lookup_kernel,
        out_shape=jax.ShapeDtypeStruct((owners, capacity, row_width), dtype),
        in_specs=[vmem, vmem],
        out_specs=vmem,
        scratch_shapes=[
            pltpu.VMEM((PAD + rows + PAD, row_width), jnp.float32),
            pltpu.SemaphoreType.DMA((DEPTH,)),
        ]
        + [pltpu.SMEM((8, LANES), jnp.int32)] * DEPTH,
        compiler_params=pltpu.CompilerParams(vmem_limit_bytes=16 * MIB),
        name="lookup_rows",
    )(incoming, table)
    returned = lax.all_to_all(replies, axes, split_axis=0, concat_axis=0, tiled=True)
    returned = returned.reshape(owners * capacity, row_width)
    embedded = pl.pallas_call(
        place_kernel,
        out_shape=jax.ShapeDtypeStruct((num_feats, list_span, row_width), dtype),
        in_specs=[hbm, vmem, vmem],
        out_specs=hbm,
        scratch_shapes=[
            pltpu.SMEM(lengths.shape, jnp.int32),
            pltpu.VMEM((PAD + owners * capacity + 2 * PAD, row_width), jnp.float32),
            pltpu.VMEM((num_feats, list_span, row_width), dtype),
            pltpu.SemaphoreType.DMA,
            pltpu.SemaphoreType.DMA,
            pltpu.SemaphoreType.DMA((DEPTH,)),
        ]
        + [pltpu.SMEM((list_span // LANES, LANES), jnp.int32)] * DEPTH,
        compiler_params=pltpu.CompilerParams(vmem_limit_bytes=20 * MIB),
        name="place_rows",
    )(pltpu.with_memory_space_constraint(lengths, pltpu.HBM), targets, returned)
    return embedded.reshape(num_users, num_feats, list_span, row_width)


def solution(mesh):
    placed = (P(("ep", "dp"), None), P(("ep", "dp"), None, None), P(), P(("ep", "dp"), None))
    return jax.shard_map(
        on_device,
        mesh=mesh,
        in_specs=placed,
        out_specs=P(("ep", "dp"), None, None, None),
        check_vma=False,
    )
```

```python
import functools

import jax
import jax.numpy as jnp
from jax import lax
from jax.experimental import pallas as pl
from jax.experimental.pallas import tpu as pltpu
from jax.sharding import PartitionSpec as P

LANES = 128
BLOCK = 256
GROUP = 16
WINDOW = 128
PAD = 8
DEPTH = 4
CHAIN = 16
MIB = 2**20


def rank_kernel(
    per_owner,
    capacity,
    len_hbm,
    slot_hbm,
    ids_hbm,
    tab_hbm,
    req_ref,
    tgt_ref,
    tab_ref,
    len_ref,
    slot_ref,
    ids_ref,
    sems,
):
    copies = [
        pltpu.make_async_copy(src, dst, sems.at[k])
        for k, (src, dst) in enumerate(
            [(len_hbm, len_ref), (slot_hbm, slot_ref), (ids_hbm, ids_ref), (tab_hbm, tab_ref)]
        )
    ]
    for copy in copies:
        copy.start()
    feats, span = ids_ref.shape
    owners = req_ref.shape[0]
    half = jnp.bfloat16
    one, zero = jnp.ones((16, BLOCK), half), jnp.zeros((16, BLOCK), half)
    row_of = lax.broadcasted_iota(jnp.int32, (16, BLOCK), 0).astype(jnp.float32)
    owner_rows = [(row_of + 16 * t).astype(half) for t in range(owners // 16)]
    rank_rows = [(row_of + (16 * t + 1)).astype(half) for t in range(capacity // 16)]
    earlier = lax.broadcasted_iota(jnp.int32, (BLOCK, BLOCK), 0)
    later = lax.broadcasted_iota(jnp.int32, (BLOCK, BLOCK), 1)
    up_to = jnp.where(earlier <= later, 1.0, 0.0).astype(half)
    lane = lax.broadcasted_iota(jnp.int32, (1, BLOCK), 1)
    for copy in copies[:3]:
        copy.wait()
    ids = ids_ref[...]
    owner = ids >> (per_owner.bit_length() - 1)
    base = (owner * capacity - 1).astype(jnp.float32)
    owner = owner.astype(jnp.float32)
    row = (ids & (per_owner - 1)) * feats
    high, low = (row >> 7).astype(jnp.float32), (row & 127).astype(jnp.float32)

    offset = [jnp.zeros((16, LANES), half) for _ in owner_rows]
    request = jnp.zeros((owners, 2 * capacity), jnp.float32)
    per_feature = span // BLOCK
    for first in range(0, feats * per_feature, CHAIN):
        hots, wanted = [], []
        for step in range(first, first + CHAIN):
            f, at = step // per_feature, step % per_feature * BLOCK

            def spread(x):
                return jnp.broadcast_to(x, (16, BLOCK)).astype(half)

            def line(x):
                return x[f : f + 1, at : at + BLOCK]

            valid = (lane + at) < len_ref[0, f]
            key = spread(jnp.where(valid, line(owner), -1.0))
            hot = [jnp.where(rows == key, one, zero) for rows in owner_rows]
            hots.append(jnp.concatenate(hot, axis=0))
            counted = jnp.dot(hots[-1], up_to, preferred_element_type=jnp.float32)
            total = jnp.broadcast_to(counted[:, BLOCK - 1 :], (owners, LANES)).astype(half)
            counted = counted.astype(half)
            picked = zero
            for t in range(len(hot)):
                at_t = slice(16 * t, 16 * t + 16)
                before = counted[at_t] + jnp.concatenate([offset[t]] * (BLOCK // LANES), axis=1)
                picked = picked + hot[t] * before
                offset[t] = offset[t] + total[at_t]
            rank = jnp.sum(picked.astype(jnp.float32), axis=0, keepdims=True)
            key, high_of, low_of = spread(rank), spread(line(high)), spread(line(low) + slot_ref[f].astype(jnp.float32))
            found = [rows == key for rows in rank_rows]
            wanted.append(
                jnp.concatenate(
                    [jnp.where(x, high_of, zero) for x in found]
                    + [jnp.where(x, low_of, zero) for x in found],
                    axis=0,
                )
            )
            place = jnp.where(valid, line(base) + rank, float(owners * capacity)).astype(jnp.int32)
            for part in range(BLOCK // LANES):
                at_line = f * (span // LANES) + at // LANES + part
                tgt_ref[at_line : at_line + 1, :] = place[:, part * LANES : (part + 1) * LANES]
        request = request + lax.dot_general(
            jnp.concatenate(hots, axis=1),
            jnp.concatenate(wanted, axis=1),
            (((1,), (1,)), ((), ())),
            preferred_element_type=jnp.float32,
        )
    asked = request[:, :capacity] * 128.0 + request[:, capacity:]
    req_ref[:, :capacity] = asked.astype(jnp.int32)
    req_ref[:, capacity:] = jnp.zeros((owners, LANES - capacity), jnp.int32)
    copies[3].wait()


def widen(dst_ref, src_ref, step=256):
    def convert(i, _):
        at = pl.multiple_of(i * step, step)
        dst_ref[pl.ds(at + PAD, step), :] = src_ref[pl.ds(at, step), :].astype(jnp.float32)
        return 0

    lax.fori_loop(0, src_ref.shape[0] // step, convert, 0)


def gather_rows(wide_ref, index_of, count):
    sublane = lax.broadcasted_iota(jnp.int32, (8, wide_ref.shape[1]), 0)
    tiles = []
    for base in range(0, count, 8):
        tile = wide_ref[pl.ds(index_of(base) + PAD, 8), :]
        for r in range(1, 8):
            tile = jnp.where(sublane == r, wide_ref[pl.ds(index_of(base + r) + (PAD - r), 8), :], tile)
        tiles.append(tile)
    return jnp.concatenate(tiles, axis=0)


def in_windows(source_ref, buffers, sems, body):
    lines = buffers[0].shape[0]
    windows = source_ref.shape[0] // lines
    depth = len(buffers)

    def fetch(w, b):
        at = pl.multiple_of(w * lines, lines)
        return pltpu.make_async_copy(source_ref.at[pl.ds(at, lines)], buffers[b], sems.at[b])

    for b in range(depth):
        fetch(b, b).start()

    def turn(k, _):
        for b in range(depth):
            w = k * depth + b
            fetch(w, b).wait()
            body(w, buffers[b])

            @pl.when(w + depth < windows)
            def _():
                fetch(w + depth, b).start()

        return 0

    return lambda: lax.fori_loop(0, windows // depth, turn, 0)


def lookup_kernel(inc_ref, tab_ref, out_ref, wide_ref, sems, *buffers):
    capacity = out_ref.shape[1]

    def window(w, index_ref):
        lines = index_ref.shape[0]
        for d in range(lines):
            for g in range(0, capacity, GROUP):
                rows = gather_rows(wide_ref, lambda r: index_ref[d, g + r], GROUP)
                out_ref[w * lines + d, g : g + GROUP, :] = rows.astype(out_ref.dtype)

    run = in_windows(inc_ref, buffers, sems, window)
    widen(wide_ref, tab_ref)
    run()


def place_kernel(len_hbm, tgt_ref, ret_ref, out_hbm, len_ref, wide, out_ref, out_sem, len_sem, sems, *buffers):
    slots = ret_ref.shape[0]
    feats, span = out_ref.shape[:2]
    lengths_copy = pltpu.make_async_copy(len_hbm, len_ref, len_sem)
    lengths_copy.start()

    def feature(f, index_ref):
        used = len_ref[0, f]
        for at in range(0, span, WINDOW):

            @pl.when(used > at)
            def _():
                for g in range(at, at + WINDOW, GROUP):
                    rows = gather_rows(
                        wide, lambda r: index_ref[(g + r) // LANES, (g + r) % LANES], GROUP
                    )
                    out_ref[f, g : g + GROUP, :] = rows.astype(out_ref.dtype)

        pltpu.make_async_copy(out_ref.at[f], out_hbm.at[f], out_sem).start()

    run = in_windows(tgt_ref, buffers, sems, feature)
    widen(wide, ret_ref)
    wide[PAD + slots :, :] = jnp.zeros((wide.shape[0] - slots - PAD, wide.shape[1]), jnp.float32)

    def clear(f, _):
        out_ref[f] = jnp.zeros(out_ref.shape[1:], out_ref.dtype)
        return 0

    lax.fori_loop(0, feats, clear, 0)
    lengths_copy.wait()
    run()
    pltpu.make_async_copy(out_ref, out_hbm, out_sem).wait()


def on_device(lengths, id_lists, feature_slots, embedding_table):
    num_users, num_feats, list_span = id_lists.shape
    rows, row_width = embedding_table.shape
    owners = lax.axis_size("ep") * lax.axis_size("dp")
    per_owner = rows // num_feats
    slot_total = num_users * num_feats * list_span
    capacity = 5 * slot_total // (4 * owners)
    axes = ("ep", "dp")
    dtype = embedding_table.dtype
    vmem = pl.BlockSpec(memory_space=pltpu.VMEM)
    hbm = pl.BlockSpec(memory_space=pltpu.HBM)
    ids = id_lists.reshape(num_feats, list_span)

    request, targets, table = pl.pallas_call(
        functools.partial(rank_kernel, per_owner, capacity),
        out_shape=(
            pltpu.VMEM((owners, LANES), jnp.int32),
            pltpu.VMEM((slot_total // LANES, LANES), jnp.int32),
            pltpu.VMEM((rows, row_width), dtype),
        ),
        in_specs=[hbm] * 4,
        out_specs=(vmem,) * 3,
        scratch_shapes=[
            pltpu.SMEM(lengths.shape, jnp.int32),
            pltpu.SMEM(feature_slots.shape, jnp.int32),
            pltpu.VMEM(ids.shape, jnp.int32),
            pltpu.SemaphoreType.DMA((4,)),
        ],
        compiler_params=pltpu.CompilerParams(
            vmem_limit_bytes=16 * MIB
        ),
        name="rank_ids",
    )(*(pltpu.with_memory_space_constraint(x, pltpu.HBM) for x in (lengths, feature_slots, ids, embedding_table)))
    incoming = lax.all_to_all(request, axes, split_axis=0, concat_axis=0, tiled=True)
    replies = pl.pallas_call(
        lookup_kernel,
        out_shape=jax.ShapeDtypeStruct((owners, capacity, row_width), dtype),
        in_specs=[vmem, vmem],
        out_specs=vmem,
        scratch_shapes=[
            pltpu.VMEM((PAD + rows + PAD, row_width), jnp.float32),
            pltpu.SemaphoreType.DMA((DEPTH,)),
        ]
        + [pltpu.SMEM((8, LANES), jnp.int32)] * DEPTH,
        compiler_params=pltpu.CompilerParams(vmem_limit_bytes=16 * MIB),
        name="lookup_rows",
    )(incoming, table)
    returned = lax.all_to_all(replies, axes, split_axis=0, concat_axis=0, tiled=True)
    returned = returned.reshape(owners * capacity, row_width)
    embedded = pl.pallas_call(
        place_kernel,
        out_shape=jax.ShapeDtypeStruct((num_feats, list_span, row_width), dtype),
        in_specs=[hbm, vmem, vmem],
        out_specs=hbm,
        scratch_shapes=[
            pltpu.SMEM(lengths.shape, jnp.int32),
            pltpu.VMEM((PAD + owners * capacity + 2 * PAD, row_width), jnp.float32),
            pltpu.VMEM((num_feats, list_span, row_width), dtype),
            pltpu.SemaphoreType.DMA,
            pltpu.SemaphoreType.DMA,
            pltpu.SemaphoreType.DMA((DEPTH,)),
        ]
        + [pltpu.SMEM((list_span // LANES, LANES), jnp.int32)] * DEPTH,
        compiler_params=pltpu.CompilerParams(vmem_limit_bytes=20 * MIB),
        name="place_rows",
    )(pltpu.with_memory_space_constraint(lengths, pltpu.HBM), targets, returned)
    return embedded.reshape(num_users, num_feats, list_span, row_width)


def solution(mesh):
    placed = (P(("ep", "dp"), None), P(("ep", "dp"), None, None), P(), P(("ep", "dp"), None))
    return jax.shard_map(
        on_device,
        mesh=mesh,
        in_specs=placed,
        out_specs=P(("ep", "dp"), None, None, None),
        check_vma=False,
    )
```

```python
import functools

import jax
import jax.numpy as jnp
from jax import lax
from jax.experimental import pallas as pl
from jax.experimental.pallas import tpu as pltpu
from jax.sharding import PartitionSpec as P

LANES = 128
BLOCK = 256
GROUP = 16
WINDOW = 128
PAD = 8
DEPTH = 2
LINES = 16
MIB = 2**20


def rank_kernel(
    per_owner,
    capacity,
    len_hbm,
    slot_hbm,
    ids_hbm,
    tab_hbm,
    req_ref,
    tgt_ref,
    tab_ref,
    len_ref,
    slot_ref,
    ids_ref,
    sems,
):
    copies = [
        pltpu.make_async_copy(src, dst, sems.at[k])
        for k, (src, dst) in enumerate(
            [(len_hbm, len_ref), (slot_hbm, slot_ref), (ids_hbm, ids_ref), (tab_hbm, tab_ref)]
        )
    ]
    for copy in copies:
        copy.start()
    feats, span = ids_ref.shape
    owners = req_ref.shape[0]
    half = jnp.bfloat16
    one, zero = jnp.ones((16, BLOCK), half), jnp.zeros((16, BLOCK), half)
    row_of = lax.broadcasted_iota(jnp.int32, (16, BLOCK), 0).astype(jnp.float32)
    owner_rows = [(row_of + 16 * t).astype(half) for t in range(owners // 16)]
    rank_rows = [(row_of + (16 * t + 1)).astype(half) for t in range(capacity // 16)]
    earlier = lax.broadcasted_iota(jnp.int32, (BLOCK, BLOCK), 0)
    later = lax.broadcasted_iota(jnp.int32, (BLOCK, BLOCK), 1)
    up_to = jnp.where(earlier <= later, 1.0, 0.0).astype(half)
    lane = lax.broadcasted_iota(jnp.int32, (1, BLOCK), 1)
    for copy in copies[:3]:
        copy.wait()
    ids = ids_ref[...]
    owner = ids >> (per_owner.bit_length() - 1)
    base = (owner * capacity - 1).astype(jnp.float32)
    owner = owner.astype(jnp.float32)
    row = (ids & (per_owner - 1)) * feats
    low = (128 + (row & 127)).astype(jnp.float32)
    high = jnp.exp2((row >> 7).astype(jnp.float32))

    offset = [jnp.zeros((16, LANES), half) for _ in owner_rows]
    request = jnp.zeros((owners, capacity), jnp.float32)
    per_feature = span // BLOCK

    def spread(x):
        return jnp.broadcast_to(x, (16, BLOCK)).astype(half)

    for step in range(feats * per_feature):
        f, at = step // per_feature, step % per_feature * BLOCK

        def line(x):
            return x[f : f + 1, at : at + BLOCK]

        valid = (lane + at) < len_ref[0, f]
        key = spread(jnp.where(valid, line(owner), -1.0))
        hot = [jnp.where(rows == key, one, zero) for rows in owner_rows]
        hot_all = jnp.concatenate(hot, axis=0)
        counted = jnp.dot(hot_all, up_to, preferred_element_type=jnp.float32)
        total = jnp.broadcast_to(counted[:, BLOCK - 1 :], (owners, LANES)).astype(half)
        counted = counted.astype(half)
        picked = zero
        for t in range(len(hot)):
            at_t = slice(16 * t, 16 * t + 16)
            before = counted[at_t] + jnp.concatenate([offset[t]] * (BLOCK // LANES), axis=1)
            picked = picked + hot[t] * before
            offset[t] = offset[t] + total[at_t]
        rank = jnp.sum(picked.astype(jnp.float32), axis=0, keepdims=True)
        key = spread(rank)
        code = spread((line(low) + slot_ref[f].astype(jnp.float32)) * line(high))
        request = request + lax.dot_general(
            hot_all,
            jnp.concatenate([jnp.where(rows == key, code, zero) for rows in rank_rows], axis=0),
            (((1,), (1,)), ((), ())),
            preferred_element_type=jnp.float32,
        )
        place = jnp.where(valid, line(base) + rank, float(owners * capacity)).astype(jnp.int32)
        for part in range(BLOCK // LANES):
            at_line = f * (span // LANES) + at // LANES + part
            tgt_ref[at_line : at_line + 1, :] = place[:, part * LANES : (part + 1) * LANES]
    request = jnp.maximum(request, 128.0)
    power = jnp.floor(jnp.log2(request) + 0.002)
    asked = (power - 7.0) * 128.0 + jnp.round(request * jnp.exp2(7.0 - power)) - 128.0
    req_ref[:, :capacity] = asked.astype(jnp.int32)
    req_ref[:, capacity:] = jnp.zeros((owners, LANES - capacity), jnp.int32)
    copies[3].wait()


def widen(dst_ref, src_ref, step=256):
    def convert(i, _):
        at = pl.multiple_of(i * step, step)
        dst_ref[pl.ds(at + PAD, step), :] = src_ref[pl.ds(at, step), :].astype(jnp.float32)
        return 0

    lax.fori_loop(0, src_ref.shape[0] // step, convert, 0)


def gather_rows(wide_ref, index_of, count):
    sublane = lax.broadcasted_iota(jnp.int32, (8, wide_ref.shape[1]), 0)
    tiles = []
    for base in range(0, count, 8):
        tile = wide_ref[pl.ds(index_of(base) + PAD, 8), :]
        for r in range(1, 8):
            tile = jnp.where(sublane == r, wide_ref[pl.ds(index_of(base + r) + (PAD - r), 8), :], tile)
        tiles.append(tile)
    return jnp.concatenate(tiles, axis=0)


def in_windows(source_ref, buffers, sems, body):
    lines = buffers[0].shape[0]
    windows = source_ref.shape[0] // lines
    depth = len(buffers)

    def fetch(w, b):
        at = pl.multiple_of(w * lines, lines)
        return pltpu.make_async_copy(source_ref.at[pl.ds(at, lines)], buffers[b], sems.at[b])

    for b in range(depth):
        fetch(b, b).start()

    def turn(k, _):
        for b in range(depth):
            w = k * depth + b
            fetch(w, b).wait()
            body(w, buffers[b])

            @pl.when(w + depth < windows)
            def _():
                fetch(w + depth, b).start()

        return 0

    return lambda: lax.fori_loop(0, windows // depth, turn, 0)


def lookup_kernel(inc_ref, tab_ref, out_ref, wide_ref, sems, *buffers):
    capacity = out_ref.shape[1]

    def window(w, index_ref):
        lines = index_ref.shape[0]
        for d in range(lines):
            for g in range(0, capacity, GROUP):
                rows = gather_rows(wide_ref, lambda r: index_ref[d, g + r], GROUP)
                out_ref[w * lines + d, g : g + GROUP, :] = rows.astype(out_ref.dtype)

    run = in_windows(inc_ref, buffers, sems, window)
    widen(wide_ref, tab_ref)
    run()


def place_kernel(len_hbm, tgt_ref, ret_ref, out_hbm, len_ref, wide, out_ref, out_sem, len_sem, sems, *buffers):
    slots = ret_ref.shape[0]
    feats, span = out_ref.shape[:2]
    lengths_copy = pltpu.make_async_copy(len_hbm, len_ref, len_sem)
    lengths_copy.start()

    def features(w, index_ref):
        lines = span // LANES
        for k in range(index_ref.shape[0] // lines):
            feature(w * (index_ref.shape[0] // lines) + k, k * lines, index_ref)

    def feature(f, line, index_ref):
        used = len_ref[0, f]
        for at in range(0, span, WINDOW):

            @pl.when(used > at)
            def _():
                for g in range(at, at + WINDOW, GROUP):
                    rows = gather_rows(
                        wide,
                        lambda r: index_ref[line + (g + r) // LANES, (g + r) % LANES],
                        GROUP,
                    )
                    out_ref[f, g : g + GROUP, :] = rows.astype(out_ref.dtype)

        pltpu.make_async_copy(out_ref.at[f], out_hbm.at[f], out_sem).start()

    run = in_windows(tgt_ref, buffers, sems, features)
    widen(wide, ret_ref)
    wide[PAD + slots :, :] = jnp.zeros((wide.shape[0] - slots - PAD, wide.shape[1]), jnp.float32)

    def clear(f, _):
        out_ref[f] = jnp.zeros(out_ref.shape[1:], out_ref.dtype)
        return 0

    lax.fori_loop(0, feats, clear, 0)
    lengths_copy.wait()
    run()
    pltpu.make_async_copy(out_ref, out_hbm, out_sem).wait()


def on_device(lengths, id_lists, feature_slots, embedding_table):
    num_users, num_feats, list_span = id_lists.shape
    rows, row_width = embedding_table.shape
    owners = lax.axis_size("ep") * lax.axis_size("dp")
    per_owner = rows // num_feats
    slot_total = num_users * num_feats * list_span
    capacity = 5 * slot_total // (4 * owners)
    axes = ("ep", "dp")
    dtype = embedding_table.dtype
    vmem = pl.BlockSpec(memory_space=pltpu.VMEM)
    hbm = pl.BlockSpec(memory_space=pltpu.HBM)
    ids = id_lists.reshape(num_feats, list_span)

    request, targets, table = pl.pallas_call(
        functools.partial(rank_kernel, per_owner, capacity),
        out_shape=(
            pltpu.VMEM((owners, LANES), jnp.int32),
            pltpu.VMEM((slot_total // LANES, LANES), jnp.int32),
            pltpu.VMEM((rows, row_width), dtype),
        ),
        in_specs=[hbm] * 4,
        out_specs=(vmem,) * 3,
        scratch_shapes=[
            pltpu.SMEM(lengths.shape, jnp.int32),
            pltpu.SMEM(feature_slots.shape, jnp.int32),
            pltpu.VMEM(ids.shape, jnp.int32),
            pltpu.SemaphoreType.DMA((4,)),
        ],
        compiler_params=pltpu.CompilerParams(vmem_limit_bytes=16 * MIB),
        name="rank_ids",
    )(*(pltpu.with_memory_space_constraint(x, pltpu.HBM) for x in (lengths, feature_slots, ids, embedding_table)))
    incoming = lax.all_to_all(request, axes, split_axis=0, concat_axis=0, tiled=True)
    replies = pl.pallas_call(
        lookup_kernel,
        out_shape=jax.ShapeDtypeStruct((owners, capacity, row_width), dtype),
        in_specs=[vmem, vmem],
        out_specs=vmem,
        scratch_shapes=[
            pltpu.VMEM((PAD + rows + PAD, row_width), jnp.float32),
            pltpu.SemaphoreType.DMA((DEPTH,)),
        ]
        + [pltpu.SMEM((LINES, LANES), jnp.int32)] * DEPTH,
        compiler_params=pltpu.CompilerParams(vmem_limit_bytes=16 * MIB),
        name="lookup_rows",
    )(incoming, table)
    returned = lax.all_to_all(replies, axes, split_axis=0, concat_axis=0, tiled=True)
    returned = returned.reshape(owners * capacity, row_width)
    embedded = pl.pallas_call(
        place_kernel,
        out_shape=jax.ShapeDtypeStruct((num_feats, list_span, row_width), dtype),
        in_specs=[hbm, vmem, vmem],
        out_specs=hbm,
        scratch_shapes=[
            pltpu.SMEM(lengths.shape, jnp.int32),
            pltpu.VMEM((PAD + owners * capacity + 2 * PAD, row_width), jnp.float32),
            pltpu.VMEM((num_feats, list_span, row_width), dtype),
            pltpu.SemaphoreType.DMA,
            pltpu.SemaphoreType.DMA,
            pltpu.SemaphoreType.DMA((DEPTH,)),
        ]
        + [pltpu.SMEM((LINES, LANES), jnp.int32)] * DEPTH,
        compiler_params=pltpu.CompilerParams(vmem_limit_bytes=20 * MIB),
        name="place_rows",
    )(pltpu.with_memory_space_constraint(lengths, pltpu.HBM), targets, returned)
    return embedded.reshape(num_users, num_feats, list_span, row_width)


def solution(mesh):
    placed = (P(("ep", "dp"), None), P(("ep", "dp"), None, None), P(), P(("ep", "dp"), None))
    return jax.shard_map(
        on_device,
        mesh=mesh,
        in_specs=placed,
        out_specs=P(("ep", "dp"), None, None, None),
        check_vma=False,
    )
```

```python
import functools

import jax
import jax.numpy as jnp
from jax import lax
from jax.experimental import pallas as pl
from jax.experimental.pallas import tpu as pltpu
from jax.sharding import PartitionSpec as P

LANES = 128
BLOCK = 256
GROUP = 16
WINDOW = 128
PAD = 8
DEPTH = 2
LINES = 16
FEW = 48
MIB = 2**20


def rank_kernel(
    per_owner,
    capacity,
    len_hbm,
    slot_hbm,
    ids_hbm,
    tab_hbm,
    req_ref,
    tgt_ref,
    tab_ref,
    len_ref,
    slot_ref,
    ids_ref,
    sems,
):
    copies = [
        pltpu.make_async_copy(src, dst, sems.at[k])
        for k, (src, dst) in enumerate(
            [(len_hbm, len_ref), (slot_hbm, slot_ref), (ids_hbm, ids_ref), (tab_hbm, tab_ref)]
        )
    ]
    for copy in copies:
        copy.start()
    feats, span = ids_ref.shape
    owners = req_ref.shape[0]
    half = jnp.bfloat16
    one, zero = jnp.ones((16, BLOCK), half), jnp.zeros((16, BLOCK), half)
    row_of = lax.broadcasted_iota(jnp.int32, (16, BLOCK), 0).astype(jnp.float32)
    owner_rows = [(row_of + 16 * t).astype(half) for t in range(owners // 16)]
    rank_rows = [(row_of + (16 * t + 1)).astype(half) for t in range(capacity // 16)]
    earlier = lax.broadcasted_iota(jnp.int32, (BLOCK, BLOCK), 0)
    later = lax.broadcasted_iota(jnp.int32, (BLOCK, BLOCK), 1)
    up_to = jnp.where(earlier <= later, 1.0, 0.0).astype(half)
    lane = lax.broadcasted_iota(jnp.int32, (1, BLOCK), 1)
    for copy in copies[:3]:
        copy.wait()
    ids = ids_ref[...]
    owner = ids >> (per_owner.bit_length() - 1)
    base = (owner * capacity - 1).astype(jnp.float32)
    owner = owner.astype(jnp.float32)
    row = (ids & (per_owner - 1)) * feats
    low = (128 + (row & 127)).astype(jnp.float32)
    high = jnp.exp2((row >> 7).astype(jnp.float32))

    offset = [jnp.zeros((16, LANES), half) for _ in owner_rows]
    request = jnp.zeros((owners, capacity), jnp.float32)
    per_feature = span // BLOCK

    def spread(x):
        return jnp.broadcast_to(x, (16, BLOCK)).astype(half)

    for step in range(feats * per_feature):
        f, at = step // per_feature, step % per_feature * BLOCK

        def line(x):
            return x[f : f + 1, at : at + BLOCK]

        valid = (lane + at) < len_ref[0, f]
        key = spread(jnp.where(valid, line(owner), -1.0))
        hot = [jnp.where(rows == key, one, zero) for rows in owner_rows]
        hot_all = jnp.concatenate(hot, axis=0)
        counted = jnp.dot(hot_all, up_to, preferred_element_type=jnp.float32)
        total = jnp.broadcast_to(counted[:, BLOCK - 1 :], (owners, LANES)).astype(half)
        counted = counted.astype(half)
        picked = zero
        for t in range(len(hot)):
            at_t = slice(16 * t, 16 * t + 16)
            before = counted[at_t] + jnp.concatenate([offset[t]] * (BLOCK // LANES), axis=1)
            picked = picked + hot[t] * before
            offset[t] = offset[t] + total[at_t]
        rank = jnp.sum(picked.astype(jnp.float32), axis=0, keepdims=True)
        key = spread(rank)
        code = spread((line(low) + slot_ref[f].astype(jnp.float32)) * line(high))
        request = request + lax.dot_general(
            hot_all,
            jnp.concatenate([jnp.where(rows == key, code, zero) for rows in rank_rows], axis=0),
            (((1,), (1,)), ((), ())),
            preferred_element_type=jnp.float32,
        )
        place = jnp.where(valid, line(base) + rank, float(owners * capacity)).astype(jnp.int32)
        for part in range(BLOCK // LANES):
            at_line = f * (span // LANES) + at // LANES + part
            tgt_ref[at_line : at_line + 1, :] = place[:, part * LANES : (part + 1) * LANES]
    request = jnp.maximum(request, 128.0)
    power = jnp.floor(jnp.log2(request) + 0.002)
    asked = (power - 7.0) * 128.0 + jnp.round(request * jnp.exp2(7.0 - power)) - 128.0
    req_ref[:, :capacity] = asked.astype(jnp.int32)
    count = jnp.concatenate([x.astype(jnp.float32) for x in offset], axis=0)
    req_ref[:, capacity:] = count[:, capacity:].astype(jnp.int32)
    copies[3].wait()


def widen(dst_ref, src_ref, step=256):
    def convert(i, _):
        at = pl.multiple_of(i * step, step)
        dst_ref[pl.ds(at + PAD, step), :] = src_ref[pl.ds(at, step), :].astype(jnp.float32)
        return 0

    lax.fori_loop(0, src_ref.shape[0] // step, convert, 0)


def gather_rows(wide_ref, index_of, count):
    sublane = lax.broadcasted_iota(jnp.int32, (8, wide_ref.shape[1]), 0)
    tiles = []
    for base in range(0, count, 8):
        tile = wide_ref[pl.ds(index_of(base) + PAD, 8), :]
        for r in range(1, 8):
            tile = jnp.where(sublane == r, wide_ref[pl.ds(index_of(base + r) + (PAD - r), 8), :], tile)
        tiles.append(tile)
    return jnp.concatenate(tiles, axis=0)


def in_windows(source_ref, buffers, sems, body):
    lines = buffers[0].shape[0]
    windows = source_ref.shape[0] // lines
    depth = len(buffers)

    def fetch(w, b):
        at = pl.multiple_of(w * lines, lines)
        return pltpu.make_async_copy(source_ref.at[pl.ds(at, lines)], buffers[b], sems.at[b])

    for b in range(depth):
        fetch(b, b).start()

    def turn(k, _):
        for b in range(depth):
            w = k * depth + b
            fetch(w, b).wait()
            body(w, buffers[b])

            @pl.when(w + depth < windows)
            def _():
                fetch(w + depth, b).start()

        return 0

    return lambda: lax.fori_loop(0, windows // depth, turn, 0)


def lookup_kernel(inc_ref, tab_ref, out_ref, wide_ref, sems, *buffers):
    capacity = out_ref.shape[1]

    def fill(w, index_ref, ranks):
        lines = index_ref.shape[0]
        for d in range(lines):
            for g in range(0, ranks, GROUP):
                rows = gather_rows(wide_ref, lambda r: index_ref[d, g + r], GROUP)
                out_ref[w * lines + d, g : g + GROUP, :] = rows.astype(out_ref.dtype)

    def window(w, index_ref):
        most = functools.reduce(
            jnp.maximum, [index_ref[d, capacity] for d in range(index_ref.shape[0])]
        )

        @pl.when(most <= FEW)
        def _():
            fill(w, index_ref, FEW)

        @pl.when(most > FEW)
        def _():
            fill(w, index_ref, capacity)

    run = in_windows(inc_ref, buffers, sems, window)
    widen(wide_ref, tab_ref)
    run()


def place_kernel(len_hbm, tgt_ref, ret_ref, out_hbm, len_ref, wide, out_ref, out_sem, len_sem, sems, *buffers):
    slots = ret_ref.shape[0]
    feats, span = out_ref.shape[:2]
    lengths_copy = pltpu.make_async_copy(len_hbm, len_ref, len_sem)
    lengths_copy.start()

    def features(w, index_ref):
        lines = span // LANES
        for k in range(index_ref.shape[0] // lines):
            feature(w * (index_ref.shape[0] // lines) + k, k * lines, index_ref)

    def feature(f, line, index_ref):
        used = len_ref[0, f]
        for at in range(0, span, WINDOW):

            @pl.when(used > at)
            def _():
                for g in range(at, at + WINDOW, GROUP):
                    rows = gather_rows(
                        wide,
                        lambda r: index_ref[line + (g + r) // LANES, (g + r) % LANES],
                        GROUP,
                    )
                    out_ref[f, g : g + GROUP, :] = rows.astype(out_ref.dtype)

        pltpu.make_async_copy(out_ref.at[f], out_hbm.at[f], out_sem).start()

    run = in_windows(tgt_ref, buffers, sems, features)
    widen(wide, ret_ref)
    wide[PAD + slots :, :] = jnp.zeros((wide.shape[0] - slots - PAD, wide.shape[1]), jnp.float32)

    def clear(f, _):
        out_ref[f] = jnp.zeros(out_ref.shape[1:], out_ref.dtype)
        return 0

    lax.fori_loop(0, feats, clear, 0)
    lengths_copy.wait()
    run()
    pltpu.make_async_copy(out_ref, out_hbm, out_sem).wait()


def on_device(lengths, id_lists, feature_slots, embedding_table):
    num_users, num_feats, list_span = id_lists.shape
    rows, row_width = embedding_table.shape
    owners = lax.axis_size("ep") * lax.axis_size("dp")
    per_owner = rows // num_feats
    slot_total = num_users * num_feats * list_span
    capacity = 5 * slot_total // (4 * owners)
    axes = ("ep", "dp")
    dtype = embedding_table.dtype
    vmem = pl.BlockSpec(memory_space=pltpu.VMEM)
    hbm = pl.BlockSpec(memory_space=pltpu.HBM)
    ids = id_lists.reshape(num_feats, list_span)

    request, targets, table = pl.pallas_call(
        functools.partial(rank_kernel, per_owner, capacity),
        out_shape=(
            pltpu.VMEM((owners, LANES), jnp.int32),
            pltpu.VMEM((slot_total // LANES, LANES), jnp.int32),
            pltpu.VMEM((rows, row_width), dtype),
        ),
        in_specs=[hbm] * 4,
        out_specs=(vmem,) * 3,
        scratch_shapes=[
            pltpu.SMEM(lengths.shape, jnp.int32),
            pltpu.SMEM(feature_slots.shape, jnp.int32),
            pltpu.VMEM(ids.shape, jnp.int32),
            pltpu.SemaphoreType.DMA((4,)),
        ],
        compiler_params=pltpu.CompilerParams(vmem_limit_bytes=16 * MIB),
        name="rank_ids",
    )(*(pltpu.with_memory_space_constraint(x, pltpu.HBM) for x in (lengths, feature_slots, ids, embedding_table)))
    incoming = lax.all_to_all(request, axes, split_axis=0, concat_axis=0, tiled=True)
    replies = pl.pallas_call(
        lookup_kernel,
        out_shape=jax.ShapeDtypeStruct((owners, capacity, row_width), dtype),
        in_specs=[vmem, vmem],
        out_specs=vmem,
        scratch_shapes=[
            pltpu.VMEM((PAD + rows + PAD, row_width), jnp.float32),
            pltpu.SemaphoreType.DMA((DEPTH,)),
        ]
        + [pltpu.SMEM((LINES, LANES), jnp.int32)] * DEPTH,
        compiler_params=pltpu.CompilerParams(vmem_limit_bytes=16 * MIB),
        name="lookup_rows",
    )(incoming, table)
    returned = lax.all_to_all(replies, axes, split_axis=0, concat_axis=0, tiled=True)
    returned = returned.reshape(owners * capacity, row_width)
    embedded = pl.pallas_call(
        place_kernel,
        out_shape=jax.ShapeDtypeStruct((num_feats, list_span, row_width), dtype),
        in_specs=[hbm, vmem, vmem],
        out_specs=hbm,
        scratch_shapes=[
            pltpu.SMEM(lengths.shape, jnp.int32),
            pltpu.VMEM((PAD + owners * capacity + 2 * PAD, row_width), jnp.float32),
            pltpu.VMEM((num_feats, list_span, row_width), dtype),
            pltpu.SemaphoreType.DMA,
            pltpu.SemaphoreType.DMA,
            pltpu.SemaphoreType.DMA((DEPTH,)),
        ]
        + [pltpu.SMEM((LINES, LANES), jnp.int32)] * DEPTH,
        compiler_params=pltpu.CompilerParams(vmem_limit_bytes=20 * MIB),
        name="place_rows",
    )(pltpu.with_memory_space_constraint(lengths, pltpu.HBM), targets, returned)
    return embedded.reshape(num_users, num_feats, list_span, row_width)


def solution(mesh):
    placed = (P(("ep", "dp"), None), P(("ep", "dp"), None, None), P(), P(("ep", "dp"), None))
    return jax.shard_map(
        on_device,
        mesh=mesh,
        in_specs=placed,
        out_specs=P(("ep", "dp"), None, None, None),
        check_vma=False,
    )
```

```python
import functools

import jax
import jax.numpy as jnp
from jax import lax
from jax.experimental import pallas as pl
from jax.experimental.pallas import tpu as pltpu
from jax.sharding import PartitionSpec as P

LANES = 128
BLOCK = 256
GROUP = 16
WINDOW = 128
PAD = 8
DEPTH = 2
LINES = 16
TIERS = (48, 64)
MIB = 2**20


def rank_kernel(
    per_owner,
    capacity,
    len_hbm,
    slot_hbm,
    ids_hbm,
    tab_hbm,
    req_ref,
    tgt_ref,
    tab_ref,
    len_ref,
    slot_ref,
    ids_ref,
    sems,
):
    copies = [
        pltpu.make_async_copy(src, dst, sems.at[k])
        for k, (src, dst) in enumerate(
            [(len_hbm, len_ref), (slot_hbm, slot_ref), (ids_hbm, ids_ref), (tab_hbm, tab_ref)]
        )
    ]
    for copy in copies:
        copy.start()
    feats, span = ids_ref.shape
    owners = req_ref.shape[0]
    half = jnp.bfloat16
    one, zero = jnp.ones((16, BLOCK), half), jnp.zeros((16, BLOCK), half)
    row_of = lax.broadcasted_iota(jnp.int32, (16, BLOCK), 0).astype(jnp.float32)
    owner_rows = [(row_of + 16 * t).astype(half) for t in range(owners // 16)]
    rank_rows = [(row_of + (16 * t + 1)).astype(half) for t in range(capacity // 16)]
    earlier = lax.broadcasted_iota(jnp.int32, (BLOCK, BLOCK), 0)
    later = lax.broadcasted_iota(jnp.int32, (BLOCK, BLOCK), 1)
    up_to = jnp.where(earlier <= later, 1.0, 0.0).astype(half)
    lane = lax.broadcasted_iota(jnp.int32, (1, BLOCK), 1)
    for copy in copies[:3]:
        copy.wait()
    ids = ids_ref[...]
    owner = ids >> (per_owner.bit_length() - 1)
    base = (owner * capacity - 1).astype(jnp.float32)
    owner = owner.astype(jnp.float32)
    row = (ids & (per_owner - 1)) * feats
    low = (128 + (row & 127)).astype(jnp.float32)
    high = jnp.exp2((row >> 7).astype(jnp.float32))

    offset = [jnp.zeros((16, LANES), half) for _ in owner_rows]
    request = jnp.zeros((owners, capacity), jnp.float32)
    per_feature = span // BLOCK

    def spread(x):
        return jnp.broadcast_to(x, (16, BLOCK)).astype(half)

    for step in range(feats * per_feature):
        f, at = step // per_feature, step % per_feature * BLOCK

        def line(x):
            return x[f : f + 1, at : at + BLOCK]

        valid = (lane + at) < len_ref[0, f]
        key = spread(jnp.where(valid, line(owner), -1.0))
        hot = [jnp.where(rows == key, one, zero) for rows in owner_rows]
        hot_all = jnp.concatenate(hot, axis=0)
        counted = jnp.dot(hot_all, up_to, preferred_element_type=jnp.float32)
        total = jnp.broadcast_to(counted[:, BLOCK - 1 :], (owners, LANES)).astype(half)
        counted = counted.astype(half)
        picked = zero
        for t in range(len(hot)):
            at_t = slice(16 * t, 16 * t + 16)
            before = counted[at_t] + jnp.concatenate([offset[t]] * (BLOCK // LANES), axis=1)
            picked = picked + hot[t] * before
            offset[t] = offset[t] + total[at_t]
        rank = jnp.sum(picked.astype(jnp.float32), axis=0, keepdims=True)
        key = spread(rank)
        code = spread((line(low) + slot_ref[f].astype(jnp.float32)) * line(high))
        request = request + lax.dot_general(
            hot_all,
            jnp.concatenate([jnp.where(rows == key, code, zero) for rows in rank_rows], axis=0),
            (((1,), (1,)), ((), ())),
            preferred_element_type=jnp.float32,
        )
        place = jnp.where(valid, line(base) + rank, float(owners * capacity)).astype(jnp.int32)
        for part in range(BLOCK // LANES):
            at_line = f * (span // LANES) + at // LANES + part
            tgt_ref[at_line : at_line + 1, :] = place[:, part * LANES : (part + 1) * LANES]
    request = jnp.maximum(request, 128.0)
    power = jnp.floor(jnp.log2(request) + 0.002)
    asked = (power - 7.0) * 128.0 + jnp.round(request * jnp.exp2(7.0 - power)) - 128.0
    req_ref[:, :capacity] = asked.astype(jnp.int32)
    count = jnp.concatenate([x.astype(jnp.float32) for x in offset], axis=0)
    req_ref[:, capacity:] = count[:, capacity:].astype(jnp.int32)
    copies[3].wait()


def widen(dst_ref, src_ref, step=256):
    def convert(i, _):
        at = pl.multiple_of(i * step, step)
        dst_ref[pl.ds(at + PAD, step), :] = src_ref[pl.ds(at, step), :].astype(jnp.float32)
        return 0

    lax.fori_loop(0, src_ref.shape[0] // step, convert, 0)


def gather_rows(wide_ref, index_of, count):
    sublane = lax.broadcasted_iota(jnp.int32, (8, wide_ref.shape[1]), 0)
    tiles = []
    for base in range(0, count, 8):
        tile = wide_ref[pl.ds(index_of(base) + PAD, 8), :]
        for r in range(1, 8):
            tile = jnp.where(sublane == r, wide_ref[pl.ds(index_of(base + r) + (PAD - r), 8), :], tile)
        tiles.append(tile)
    return jnp.concatenate(tiles, axis=0)


def in_windows(source_ref, buffers, sems, body):
    lines = buffers[0].shape[0]
    windows = source_ref.shape[0] // lines
    depth = len(buffers)

    def fetch(w, b):
        at = pl.multiple_of(w * lines, lines)
        return pltpu.make_async_copy(source_ref.at[pl.ds(at, lines)], buffers[b], sems.at[b])

    for b in range(depth):
        fetch(b, b).start()

    def turn(k, _):
        for b in range(depth):
            w = k * depth + b
            fetch(w, b).wait()
            body(w, buffers[b])

            @pl.when(w + depth < windows)
            def _():
                fetch(w + depth, b).start()

        return 0

    return lambda: lax.fori_loop(0, windows // depth, turn, 0)


def lookup_kernel(inc_ref, tab_ref, out_ref, wide_ref, sems, *buffers):
    capacity = out_ref.shape[1]

    def fill(w, index_ref, ranks):
        lines = index_ref.shape[0]
        for d in range(lines):
            for g in range(0, ranks, GROUP):
                rows = gather_rows(wide_ref, lambda r: index_ref[d, g + r], GROUP)
                out_ref[w * lines + d, g : g + GROUP, :] = rows.astype(out_ref.dtype)

    def window(w, index_ref):
        most = functools.reduce(
            jnp.maximum, [index_ref[d, capacity] for d in range(index_ref.shape[0])]
        )

        floor = -1
        for ranks in TIERS + (capacity,):

            @pl.when((most > floor) & ((most <= ranks) | (ranks == capacity)))
            def _():
                fill(w, index_ref, ranks)

            floor = ranks

    run = in_windows(inc_ref, buffers, sems, window)
    widen(wide_ref, tab_ref)
    run()


def place_kernel(len_hbm, tgt_ref, ret_ref, out_hbm, len_ref, wide, out_ref, out_sem, len_sem, sems, *buffers):
    slots = ret_ref.shape[0]
    feats, span = out_ref.shape[:2]
    lengths_copy = pltpu.make_async_copy(len_hbm, len_ref, len_sem)
    lengths_copy.start()

    def features(w, index_ref):
        lines = span // LANES
        for k in range(index_ref.shape[0] // lines):
            feature(w * (index_ref.shape[0] // lines) + k, k * lines, index_ref)

    def feature(f, line, index_ref):
        used = len_ref[0, f]
        for at in range(0, span, WINDOW):

            @pl.when(used > at)
            def _():
                for g in range(at, at + WINDOW, GROUP):
                    rows = gather_rows(
                        wide,
                        lambda r: index_ref[line + (g + r) // LANES, (g + r) % LANES],
                        GROUP,
                    )
                    out_ref[f, g : g + GROUP, :] = rows.astype(out_ref.dtype)

        pltpu.make_async_copy(out_ref.at[f], out_hbm.at[f], out_sem).start()

    run = in_windows(tgt_ref, buffers, sems, features)
    widen(wide, ret_ref)
    wide[PAD + slots :, :] = jnp.zeros((wide.shape[0] - slots - PAD, wide.shape[1]), jnp.float32)

    def clear(f, _):
        out_ref[f] = jnp.zeros(out_ref.shape[1:], out_ref.dtype)
        return 0

    lax.fori_loop(0, feats, clear, 0)
    lengths_copy.wait()
    run()
    pltpu.make_async_copy(out_ref, out_hbm, out_sem).wait()


def on_device(lengths, id_lists, feature_slots, embedding_table):
    num_users, num_feats, list_span = id_lists.shape
    rows, row_width = embedding_table.shape
    owners = lax.axis_size("ep") * lax.axis_size("dp")
    per_owner = rows // num_feats
    slot_total = num_users * num_feats * list_span
    capacity = 5 * slot_total // (4 * owners)
    axes = ("ep", "dp")
    dtype = embedding_table.dtype
    vmem = pl.BlockSpec(memory_space=pltpu.VMEM)
    hbm = pl.BlockSpec(memory_space=pltpu.HBM)
    ids = id_lists.reshape(num_feats, list_span)

    request, targets, table = pl.pallas_call(
        functools.partial(rank_kernel, per_owner, capacity),
        out_shape=(
            pltpu.VMEM((owners, LANES), jnp.int32),
            pltpu.VMEM((slot_total // LANES, LANES), jnp.int32),
            pltpu.VMEM((rows, row_width), dtype),
        ),
        in_specs=[hbm] * 4,
        out_specs=(vmem,) * 3,
        scratch_shapes=[
            pltpu.SMEM(lengths.shape, jnp.int32),
            pltpu.SMEM(feature_slots.shape, jnp.int32),
            pltpu.VMEM(ids.shape, jnp.int32),
            pltpu.SemaphoreType.DMA((4,)),
        ],
        compiler_params=pltpu.CompilerParams(vmem_limit_bytes=16 * MIB),
        name="rank_ids",
    )(*(pltpu.with_memory_space_constraint(x, pltpu.HBM) for x in (lengths, feature_slots, ids, embedding_table)))
    incoming = lax.all_to_all(request, axes, split_axis=0, concat_axis=0, tiled=True)
    replies = pl.pallas_call(
        lookup_kernel,
        out_shape=jax.ShapeDtypeStruct((owners, capacity, row_width), dtype),
        in_specs=[vmem, vmem],
        out_specs=vmem,
        scratch_shapes=[
            pltpu.VMEM((PAD + rows + PAD, row_width), jnp.float32),
            pltpu.SemaphoreType.DMA((DEPTH,)),
        ]
        + [pltpu.SMEM((LINES, LANES), jnp.int32)] * DEPTH,
        compiler_params=pltpu.CompilerParams(vmem_limit_bytes=16 * MIB),
        name="lookup_rows",
    )(incoming, table)
    returned = lax.all_to_all(replies, axes, split_axis=0, concat_axis=0, tiled=True)
    returned = returned.reshape(owners * capacity, row_width)
    embedded = pl.pallas_call(
        place_kernel,
        out_shape=jax.ShapeDtypeStruct((num_feats, list_span, row_width), dtype),
        in_specs=[hbm, vmem, vmem],
        out_specs=hbm,
        scratch_shapes=[
            pltpu.SMEM(lengths.shape, jnp.int32),
            pltpu.VMEM((PAD + owners * capacity + 2 * PAD, row_width), jnp.float32),
            pltpu.VMEM((num_feats, list_span, row_width), dtype),
            pltpu.SemaphoreType.DMA,
            pltpu.SemaphoreType.DMA,
            pltpu.SemaphoreType.DMA((DEPTH,)),
        ]
        + [pltpu.SMEM((LINES, LANES), jnp.int32)] * DEPTH,
        compiler_params=pltpu.CompilerParams(vmem_limit_bytes=20 * MIB),
        name="place_rows",
    )(pltpu.with_memory_space_constraint(lengths, pltpu.HBM), targets, returned)
    return embedded.reshape(num_users, num_feats, list_span, row_width)


def solution(mesh):
    placed = (P(("ep", "dp"), None), P(("ep", "dp"), None, None), P(), P(("ep", "dp"), None))
    return jax.shard_map(
        on_device,
        mesh=mesh,
        in_specs=placed,
        out_specs=P(("ep", "dp"), None, None, None),
        check_vma=False,
    )
```

```python
import functools

import jax
import jax.numpy as jnp
from jax import lax
from jax.experimental import pallas as pl
from jax.experimental.pallas import tpu as pltpu
from jax.sharding import PartitionSpec as P

LANES = 128
BLOCK = 256
GROUP = 16
WINDOW = 128
PAD = 8
DEPTH = 2
LINES = 16
FEW = 48
MIB = 2**20


def rank_kernel(
    per_owner,
    capacity,
    len_hbm,
    slot_hbm,
    ids_hbm,
    tab_hbm,
    req_ref,
    tgt_ref,
    tab_ref,
    len_ref,
    slot_ref,
    ids_ref,
    sems,
):
    copies = [
        pltpu.make_async_copy(src, dst, sems.at[k])
        for k, (src, dst) in enumerate(
            [(len_hbm, len_ref), (slot_hbm, slot_ref), (ids_hbm, ids_ref), (tab_hbm, tab_ref)]
        )
    ]
    for copy in copies:
        copy.start()
    feats, span = ids_ref.shape
    owners = req_ref.shape[0]
    half = jnp.bfloat16
    one, zero = jnp.ones((16, BLOCK), half), jnp.zeros((16, BLOCK), half)
    row_of = lax.broadcasted_iota(jnp.int32, (16, BLOCK), 0).astype(jnp.float32)
    owner_rows = [(row_of + 16 * t).astype(half) for t in range(owners // 16)]
    rank_rows = [(row_of + (16 * t + 1)).astype(half) for t in range(capacity // 16)]
    earlier = lax.broadcasted_iota(jnp.int32, (BLOCK, BLOCK), 0)
    later = lax.broadcasted_iota(jnp.int32, (BLOCK, BLOCK), 1)
    up_to = jnp.where(earlier <= later, 1.0, 0.0).astype(half)
    lane = lax.broadcasted_iota(jnp.int32, (1, BLOCK), 1)
    for copy in copies[:3]:
        copy.wait()
    ids = ids_ref[...]
    owner = ids >> (per_owner.bit_length() - 1)
    base = (owner * capacity - 1).astype(jnp.float32)
    owner = owner.astype(jnp.float32)
    row = (ids & (per_owner - 1)) * feats
    low = (128 + (row & 127)).astype(jnp.float32)
    high = jnp.exp2((row >> 7).astype(jnp.float32))

    offset = [jnp.zeros((16, LANES), half) for _ in owner_rows]
    request = jnp.zeros((owners, capacity), jnp.float32)
    per_feature = span // BLOCK

    def spread(x):
        return jnp.broadcast_to(x, (16, BLOCK)).astype(half)

    for step in range(feats * per_feature):
        f, at = step // per_feature, step % per_feature * BLOCK

        def line(x):
            return x[f : f + 1, at : at + BLOCK]

        valid = (lane + at) < len_ref[0, f]
        key = spread(jnp.where(valid, line(owner), -1.0))
        hot = [jnp.where(rows == key, one, zero) for rows in owner_rows]
        hot_all = jnp.concatenate(hot, axis=0)
        counted = jnp.dot(hot_all, up_to, preferred_element_type=jnp.float32)
        total = jnp.broadcast_to(counted[:, BLOCK - 1 :], (owners, LANES)).astype(half)
        counted = counted.astype(half)
        picked = zero
        for t in range(len(hot)):
            at_t = slice(16 * t, 16 * t + 16)
            before = counted[at_t] + jnp.concatenate([offset[t]] * (BLOCK // LANES), axis=1)
            picked = picked + hot[t] * before
            offset[t] = offset[t] + total[at_t]
        rank = jnp.sum(picked.astype(jnp.float32), axis=0, keepdims=True)
        key = spread(rank)
        code = spread((line(low) + slot_ref[f].astype(jnp.float32)) * line(high))
        request = request + lax.dot_general(
            hot_all,
            jnp.concatenate([jnp.where(rows == key, code, zero) for rows in rank_rows], axis=0),
            (((1,), (1,)), ((), ())),
            preferred_element_type=jnp.float32,
        )
        place = jnp.where(valid, line(base) + rank, float(owners * capacity)).astype(jnp.int32)
        for part in range(BLOCK // LANES):
            at_line = f * (span // LANES) + at // LANES + part
            tgt_ref[at_line : at_line + 1, :] = place[:, part * LANES : (part + 1) * LANES]
    request = jnp.maximum(request, 128.0)
    power = jnp.floor(jnp.log2(request) + 0.002)
    asked = (power - 7.0) * 128.0 + jnp.round(request * jnp.exp2(7.0 - power)) - 128.0
    req_ref[:, :capacity] = asked.astype(jnp.int32)
    count = jnp.concatenate([x.astype(jnp.float32) for x in offset], axis=0)
    req_ref[:, capacity:] = count[:, capacity:].astype(jnp.int32)
    copies[3].wait()


def widen(dst_ref, src_ref, step=256):
    def convert(i, _):
        at = pl.multiple_of(i * step, step)
        dst_ref[pl.ds(at + PAD, step), :] = src_ref[pl.ds(at, step), :].astype(jnp.float32)
        return 0

    lax.fori_loop(0, src_ref.shape[0] // step, convert, 0)


def gather_rows(wide_ref, index_of, count):
    sublane = lax.broadcasted_iota(jnp.int32, (8, wide_ref.shape[1]), 0)
    tiles = []
    for base in range(0, count, 8):
        tile = wide_ref[pl.ds(index_of(base) + PAD, 8), :]
        for r in range(1, 8):
            tile = jnp.where(sublane == r, wide_ref[pl.ds(index_of(base + r) + (PAD - r), 8), :], tile)
        tiles.append(tile)
    return jnp.concatenate(tiles, axis=0)


def in_windows(source_ref, buffers, sems, body):
    lines = buffers[0].shape[0]
    windows = source_ref.shape[0] // lines
    depth = len(buffers)

    def fetch(w, b):
        at = pl.multiple_of(w * lines, lines)
        return pltpu.make_async_copy(source_ref.at[pl.ds(at, lines)], buffers[b], sems.at[b])

    for b in range(depth):
        fetch(b, b).start()

    def turn(k, _):
        for b in range(depth):
            w = k * depth + b
            fetch(w, b).wait()
            body(w, buffers[b])

            @pl.when(w + depth < windows)
            def _():
                fetch(w + depth, b).start()

        return 0

    return lambda: lax.fori_loop(0, windows // depth, turn, 0)


def lookup_kernel(inc_ref, tab_ref, out_ref, wide_ref, peak_ref, peaks, peak_sem, sems, *buffers):
    capacity = out_ref.shape[1]

    def fill(w, index_ref, ranks):
        lines = index_ref.shape[0]
        for d in range(lines):
            for g in range(0, ranks, GROUP):
                rows = gather_rows(wide_ref, lambda r: index_ref[d, g + r], GROUP)
                out_ref[w * lines + d, g : g + GROUP, :] = rows.astype(out_ref.dtype)

    def window(w, index_ref):
        most = peaks[w, capacity]

        @pl.when(most <= FEW)
        def _():
            fill(w, index_ref, FEW)

        @pl.when(most > FEW)
        def _():
            fill(w, index_ref, capacity)

    run = in_windows(inc_ref, buffers, sems, window)
    lines = buffers[0].shape[0]
    for w in range(peak_ref.shape[0]):
        peak_ref[w : w + 1, :] = jnp.max(
            inc_ref[w * lines : (w + 1) * lines, :], axis=0, keepdims=True
        )
    peaks_copy = pltpu.make_async_copy(peak_ref, peaks, peak_sem)
    peaks_copy.start()
    widen(wide_ref, tab_ref)
    peaks_copy.wait()
    run()


def place_kernel(len_hbm, tgt_ref, ret_ref, out_hbm, len_ref, wide, out_ref, out_sem, len_sem, sems, *buffers):
    slots = ret_ref.shape[0]
    feats, span = out_ref.shape[:2]
    lengths_copy = pltpu.make_async_copy(len_hbm, len_ref, len_sem)
    lengths_copy.start()

    def features(w, index_ref):
        lines = span // LANES
        for k in range(index_ref.shape[0] // lines):
            feature(w * (index_ref.shape[0] // lines) + k, k * lines, index_ref)

    def feature(f, line, index_ref):
        used = len_ref[0, f]
        for at in range(0, span, WINDOW):

            @pl.when(used > at)
            def _():
                for g in range(at, at + WINDOW, GROUP):
                    rows = gather_rows(
                        wide,
                        lambda r: index_ref[line + (g + r) // LANES, (g + r) % LANES],
                        GROUP,
                    )
                    out_ref[f, g : g + GROUP, :] = rows.astype(out_ref.dtype)

        pltpu.make_async_copy(out_ref.at[f], out_hbm.at[f], out_sem).start()

    run = in_windows(tgt_ref, buffers, sems, features)
    widen(wide, ret_ref)
    wide[PAD + slots :, :] = jnp.zeros((wide.shape[0] - slots - PAD, wide.shape[1]), jnp.float32)

    def clear(f, _):
        out_ref[f] = jnp.zeros(out_ref.shape[1:], out_ref.dtype)
        return 0

    lax.fori_loop(0, feats, clear, 0)
    lengths_copy.wait()
    run()
    pltpu.make_async_copy(out_ref, out_hbm, out_sem).wait()


def on_device(lengths, id_lists, feature_slots, embedding_table):
    num_users, num_feats, list_span = id_lists.shape
    rows, row_width = embedding_table.shape
    owners = lax.axis_size("ep") * lax.axis_size("dp")
    per_owner = rows // num_feats
    slot_total = num_users * num_feats * list_span
    capacity = 5 * slot_total // (4 * owners)
    axes = ("ep", "dp")
    dtype = embedding_table.dtype
    vmem = pl.BlockSpec(memory_space=pltpu.VMEM)
    hbm = pl.BlockSpec(memory_space=pltpu.HBM)
    ids = id_lists.reshape(num_feats, list_span)

    request, targets, table = pl.pallas_call(
        functools.partial(rank_kernel, per_owner, capacity),
        out_shape=(
            pltpu.VMEM((owners, LANES), jnp.int32),
            pltpu.VMEM((slot_total // LANES, LANES), jnp.int32),
            pltpu.VMEM((rows, row_width), dtype),
        ),
        in_specs=[hbm] * 4,
        out_specs=(vmem,) * 3,
        scratch_shapes=[
            pltpu.SMEM(lengths.shape, jnp.int32),
            pltpu.SMEM(feature_slots.shape, jnp.int32),
            pltpu.VMEM(ids.shape, jnp.int32),
            pltpu.SemaphoreType.DMA((4,)),
        ],
        compiler_params=pltpu.CompilerParams(vmem_limit_bytes=16 * MIB),
        name="rank_ids",
    )(*(pltpu.with_memory_space_constraint(x, pltpu.HBM) for x in (lengths, feature_slots, ids, embedding_table)))
    incoming = lax.all_to_all(request, axes, split_axis=0, concat_axis=0, tiled=True)
    replies = pl.pallas_call(
        lookup_kernel,
        out_shape=jax.ShapeDtypeStruct((owners, capacity, row_width), dtype),
        in_specs=[vmem, vmem],
        out_specs=vmem,
        scratch_shapes=[
            pltpu.VMEM((PAD + rows + PAD, row_width), jnp.float32),
            pltpu.VMEM((owners // LINES, LANES), jnp.int32),
            pltpu.SMEM((owners // LINES, LANES), jnp.int32),
            pltpu.SemaphoreType.DMA,
            pltpu.SemaphoreType.DMA((DEPTH,)),
        ]
        + [pltpu.SMEM((LINES, LANES), jnp.int32)] * DEPTH,
        compiler_params=pltpu.CompilerParams(vmem_limit_bytes=16 * MIB),
        name="lookup_rows",
    )(incoming, table)
    returned = lax.all_to_all(replies, axes, split_axis=0, concat_axis=0, tiled=True)
    returned = returned.reshape(owners * capacity, row_width)
    embedded = pl.pallas_call(
        place_kernel,
        out_shape=jax.ShapeDtypeStruct((num_feats, list_span, row_width), dtype),
        in_specs=[hbm, vmem, vmem],
        out_specs=hbm,
        scratch_shapes=[
            pltpu.SMEM(lengths.shape, jnp.int32),
            pltpu.VMEM((PAD + owners * capacity + 2 * PAD, row_width), jnp.float32),
            pltpu.VMEM((num_feats, list_span, row_width), dtype),
            pltpu.SemaphoreType.DMA,
            pltpu.SemaphoreType.DMA,
            pltpu.SemaphoreType.DMA((DEPTH,)),
        ]
        + [pltpu.SMEM((LINES, LANES), jnp.int32)] * DEPTH,
        compiler_params=pltpu.CompilerParams(vmem_limit_bytes=20 * MIB),
        name="place_rows",
    )(pltpu.with_memory_space_constraint(lengths, pltpu.HBM), targets, returned)
    return embedded.reshape(num_users, num_feats, list_span, row_width)


def solution(mesh):
    placed = (P(("ep", "dp"), None), P(("ep", "dp"), None, None), P(), P(("ep", "dp"), None))
    return jax.shard_map(
        on_device,
        mesh=mesh,
        in_specs=placed,
        out_specs=P(("ep", "dp"), None, None, None),
        check_vma=False,
    )
```

```python
import functools

import jax
import jax.numpy as jnp
from jax import lax
from jax.experimental import pallas as pl
from jax.experimental.pallas import tpu as pltpu
from jax.sharding import PartitionSpec as P

LANES = 128
BLOCK = 256
GROUP = 16
WINDOW = 128
PAD = 8
DEPTH = 2
LINES = 16
ASK_DEPTH = 4
ASK_LINES = 8
FEW = 48
MIB = 2**20


def rank_kernel(
    per_owner,
    capacity,
    len_hbm,
    slot_hbm,
    ids_hbm,
    tab_hbm,
    req_ref,
    tgt_ref,
    tab_ref,
    len_ref,
    slot_ref,
    ids_ref,
    sems,
):
    copies = [
        pltpu.make_async_copy(src, dst, sems.at[k])
        for k, (src, dst) in enumerate(
            [(len_hbm, len_ref), (slot_hbm, slot_ref), (ids_hbm, ids_ref), (tab_hbm, tab_ref)]
        )
    ]
    for copy in copies:
        copy.start()
    feats, span = ids_ref.shape
    owners = req_ref.shape[0]
    half = jnp.bfloat16
    one, zero = jnp.ones((16, BLOCK), half), jnp.zeros((16, BLOCK), half)
    row_of = lax.broadcasted_iota(jnp.int32, (16, BLOCK), 0).astype(jnp.float32)
    owner_rows = [(row_of + 16 * t).astype(half) for t in range(owners // 16)]
    rank_rows = [(row_of + (16 * t + 1)).astype(half) for t in range(capacity // 16)]
    earlier = lax.broadcasted_iota(jnp.int32, (BLOCK, BLOCK), 0)
    later = lax.broadcasted_iota(jnp.int32, (BLOCK, BLOCK), 1)
    up_to = jnp.where(earlier <= later, 1.0, 0.0).astype(half)
    lane = lax.broadcasted_iota(jnp.int32, (1, BLOCK), 1)
    for copy in copies[:3]:
        copy.wait()
    ids = ids_ref[...]
    owner = ids >> (per_owner.bit_length() - 1)
    base = (owner * capacity - 1).astype(jnp.float32)
    owner = owner.astype(jnp.float32)
    row = (ids & (per_owner - 1)) * feats
    low = (128 + (row & 127)).astype(jnp.float32)
    high = jnp.exp2((row >> 7).astype(jnp.float32))

    offset = [jnp.zeros((16, LANES), half) for _ in owner_rows]
    request = jnp.zeros((owners, capacity), jnp.float32)
    per_feature = span // BLOCK

    def spread(x):
        return jnp.broadcast_to(x, (16, BLOCK)).astype(half)

    for step in range(feats * per_feature):
        f, at = step // per_feature, step % per_feature * BLOCK

        def line(x):
            return x[f : f + 1, at : at + BLOCK]

        valid = (lane + at) < len_ref[0, f]
        key = spread(jnp.where(valid, line(owner), -1.0))
        hot = [jnp.where(rows == key, one, zero) for rows in owner_rows]
        hot_all = jnp.concatenate(hot, axis=0)
        counted = jnp.dot(hot_all, up_to, preferred_element_type=jnp.float32)
        total = jnp.broadcast_to(counted[:, BLOCK - 1 :], (owners, LANES)).astype(half)
        counted = counted.astype(half)
        picked = zero
        for t in range(len(hot)):
            at_t = slice(16 * t, 16 * t + 16)
            before = counted[at_t] + jnp.concatenate([offset[t]] * (BLOCK // LANES), axis=1)
            picked = picked + hot[t] * before
            offset[t] = offset[t] + total[at_t]
        rank = jnp.sum(picked.astype(jnp.float32), axis=0, keepdims=True)
        key = spread(rank)
        code = spread((line(low) + slot_ref[f].astype(jnp.float32)) * line(high))
        request = request + lax.dot_general(
            hot_all,
            jnp.concatenate([jnp.where(rows == key, code, zero) for rows in rank_rows], axis=0),
            (((1,), (1,)), ((), ())),
            preferred_element_type=jnp.float32,
        )
        place = jnp.where(valid, line(base) + rank, float(owners * capacity)).astype(jnp.int32)
        for part in range(BLOCK // LANES):
            at_line = f * (span // LANES) + at // LANES + part
            tgt_ref[at_line : at_line + 1, :] = place[:, part * LANES : (part + 1) * LANES]
    request = jnp.maximum(request, 128.0)
    power = jnp.floor(jnp.log2(request) + 0.002)
    asked = (power - 7.0) * 128.0 + jnp.round(request * jnp.exp2(7.0 - power)) - 128.0
    req_ref[:, :capacity] = asked.astype(jnp.int32)
    count = jnp.concatenate([x.astype(jnp.float32) for x in offset], axis=0)
    req_ref[:, capacity:] = count[:, capacity:].astype(jnp.int32)
    copies[3].wait()


def widen(dst_ref, src_ref, step=256):
    def convert(i, _):
        at = pl.multiple_of(i * step, step)
        dst_ref[pl.ds(at + PAD, step), :] = src_ref[pl.ds(at, step), :].astype(jnp.float32)
        return 0

    lax.fori_loop(0, src_ref.shape[0] // step, convert, 0)


def gather_rows(wide_ref, index_of, count):
    sublane = lax.broadcasted_iota(jnp.int32, (8, wide_ref.shape[1]), 0)
    tiles = []
    for base in range(0, count, 8):
        tile = wide_ref[pl.ds(index_of(base) + PAD, 8), :]
        for r in range(1, 8):
            tile = jnp.where(sublane == r, wide_ref[pl.ds(index_of(base + r) + (PAD - r), 8), :], tile)
        tiles.append(tile)
    return jnp.concatenate(tiles, axis=0)


def in_windows(source_ref, buffers, sems, body):
    lines = buffers[0].shape[0]
    windows = source_ref.shape[0] // lines
    depth = len(buffers)

    def fetch(w, b):
        at = pl.multiple_of(w * lines, lines)
        return pltpu.make_async_copy(source_ref.at[pl.ds(at, lines)], buffers[b], sems.at[b])

    for b in range(depth):
        fetch(b, b).start()

    def turn(k, _):
        for b in range(depth):
            w = k * depth + b
            fetch(w, b).wait()
            body(w, buffers[b])

            @pl.when(w + depth < windows)
            def _():
                fetch(w + depth, b).start()

        return 0

    return lambda: lax.fori_loop(0, windows // depth, turn, 0)


def lookup_kernel(inc_ref, tab_ref, out_ref, wide_ref, peak_ref, peaks, peak_sem, sems, *buffers):
    capacity = out_ref.shape[1]

    def fill(w, index_ref, ranks):
        lines = index_ref.shape[0]
        for d in range(lines):
            for g in range(0, ranks, GROUP):
                rows = gather_rows(wide_ref, lambda r: index_ref[d, g + r], GROUP)
                out_ref[w * lines + d, g : g + GROUP, :] = rows.astype(out_ref.dtype)

    def window(w, index_ref):
        most = peaks[w, capacity]

        @pl.when(most <= FEW)
        def _():
            fill(w, index_ref, FEW)

        @pl.when(most > FEW)
        def _():
            fill(w, index_ref, capacity)

    run = in_windows(inc_ref, buffers, sems, window)
    lines = buffers[0].shape[0]
    for w in range(peak_ref.shape[0]):
        peak_ref[w : w + 1, :] = jnp.max(
            inc_ref[w * lines : (w + 1) * lines, :], axis=0, keepdims=True
        )
    peaks_copy = pltpu.make_async_copy(peak_ref, peaks, peak_sem)
    peaks_copy.start()
    widen(wide_ref, tab_ref)
    peaks_copy.wait()
    run()


def place_kernel(len_hbm, tgt_ref, ret_ref, out_hbm, len_ref, wide, out_ref, out_sem, len_sem, sems, *buffers):
    slots = ret_ref.shape[0]
    feats, span = out_ref.shape[:2]
    lengths_copy = pltpu.make_async_copy(len_hbm, len_ref, len_sem)
    lengths_copy.start()

    def features(w, index_ref):
        lines = span // LANES
        for k in range(index_ref.shape[0] // lines):
            feature(w * (index_ref.shape[0] // lines) + k, k * lines, index_ref)

    def feature(f, line, index_ref):
        used = len_ref[0, f]
        for at in range(0, span, WINDOW):

            @pl.when(used > at)
            def _():
                for g in range(at, at + WINDOW, GROUP):
                    rows = gather_rows(
                        wide,
                        lambda r: index_ref[line + (g + r) // LANES, (g + r) % LANES],
                        GROUP,
                    )
                    out_ref[f, g : g + GROUP, :] = rows.astype(out_ref.dtype)

        pltpu.make_async_copy(out_ref.at[f], out_hbm.at[f], out_sem).start()

    run = in_windows(tgt_ref, buffers, sems, features)
    widen(wide, ret_ref)
    wide[PAD + slots :, :] = jnp.zeros((wide.shape[0] - slots - PAD, wide.shape[1]), jnp.float32)

    def clear(f, _):
        out_ref[f] = jnp.zeros(out_ref.shape[1:], out_ref.dtype)
        return 0

    lax.fori_loop(0, feats, clear, 0)
    lengths_copy.wait()
    run()
    pltpu.make_async_copy(out_ref, out_hbm, out_sem).wait()


def on_device(lengths, id_lists, feature_slots, embedding_table):
    num_users, num_feats, list_span = id_lists.shape
    rows, row_width = embedding_table.shape
    owners = lax.axis_size("ep") * lax.axis_size("dp")
    per_owner = rows // num_feats
    slot_total = num_users * num_feats * list_span
    capacity = 5 * slot_total // (4 * owners)
    axes = ("ep", "dp")
    dtype = embedding_table.dtype
    vmem = pl.BlockSpec(memory_space=pltpu.VMEM)
    hbm = pl.BlockSpec(memory_space=pltpu.HBM)
    ids = id_lists.reshape(num_feats, list_span)

    request, targets, table = pl.pallas_call(
        functools.partial(rank_kernel, per_owner, capacity),
        out_shape=(
            pltpu.VMEM((owners, LANES), jnp.int32),
            pltpu.VMEM((slot_total // LANES, LANES), jnp.int32),
            pltpu.VMEM((rows, row_width), dtype),
        ),
        in_specs=[hbm] * 4,
        out_specs=(vmem,) * 3,
        scratch_shapes=[
            pltpu.SMEM(lengths.shape, jnp.int32),
            pltpu.SMEM(feature_slots.shape, jnp.int32),
            pltpu.VMEM(ids.shape, jnp.int32),
            pltpu.SemaphoreType.DMA((4,)),
        ],
        compiler_params=pltpu.CompilerParams(vmem_limit_bytes=16 * MIB),
        name="rank_ids",
    )(*(pltpu.with_memory_space_constraint(x, pltpu.HBM) for x in (lengths, feature_slots, ids, embedding_table)))
    incoming = lax.all_to_all(request, axes, split_axis=0, concat_axis=0, tiled=True)
    replies = pl.pallas_call(
        lookup_kernel,
        out_shape=jax.ShapeDtypeStruct((owners, capacity, row_width), dtype),
        in_specs=[vmem, vmem],
        out_specs=vmem,
        scratch_shapes=[
            pltpu.VMEM((PAD + rows + PAD, row_width), jnp.float32),
            pltpu.VMEM((owners // ASK_LINES, LANES), jnp.int32),
            pltpu.SMEM((owners // ASK_LINES, LANES), jnp.int32),
            pltpu.SemaphoreType.DMA,
            pltpu.SemaphoreType.DMA((ASK_DEPTH,)),
        ]
        + [pltpu.SMEM((ASK_LINES, LANES), jnp.int32)] * ASK_DEPTH,
        compiler_params=pltpu.CompilerParams(vmem_limit_bytes=16 * MIB),
        name="lookup_rows",
    )(incoming, table)
    returned = lax.all_to_all(replies, axes, split_axis=0, concat_axis=0, tiled=True)
    returned = returned.reshape(owners * capacity, row_width)
    embedded = pl.pallas_call(
        place_kernel,
        out_shape=jax.ShapeDtypeStruct((num_feats, list_span, row_width), dtype),
        in_specs=[hbm, vmem, vmem],
        out_specs=hbm,
        scratch_shapes=[
            pltpu.SMEM(lengths.shape, jnp.int32),
            pltpu.VMEM((PAD + owners * capacity + 2 * PAD, row_width), jnp.float32),
            pltpu.VMEM((num_feats, list_span, row_width), dtype),
            pltpu.SemaphoreType.DMA,
            pltpu.SemaphoreType.DMA,
            pltpu.SemaphoreType.DMA((DEPTH,)),
        ]
        + [pltpu.SMEM((LINES, LANES), jnp.int32)] * DEPTH,
        compiler_params=pltpu.CompilerParams(vmem_limit_bytes=20 * MIB),
        name="place_rows",
    )(pltpu.with_memory_space_constraint(lengths, pltpu.HBM), targets, returned)
    return embedded.reshape(num_users, num_feats, list_span, row_width)


def solution(mesh):
    placed = (P(("ep", "dp"), None), P(("ep", "dp"), None, None), P(), P(("ep", "dp"), None))
    return jax.shard_map(
        on_device,
        mesh=mesh,
        in_specs=placed,
        out_specs=P(("ep", "dp"), None, None, None),
        check_vma=False,
    )
```
